32 devices in a mesh: mem: 4 (over y, core), lat: 4 (over z), lon: 2 (over x).
Axes of the slice: x: 2, y: 2, z: 4, core: 2. Of those that a mesh axis runs over, the one named last changes fastest.
Arguments:
- fields: bfloat16 [4, 2, 96, 96, 512], P('mem', None, 'lat', 'lon'), may hold values from -6 to 6
- region: int32 [96, 96], P('lat', 'lon'), may hold values from 0 to 2
- gain_attn: float32 [512], replicated, may hold values from 0.1 to 1.9
- w_qkv: bfloat16 [512, 1536], P(None, ('mem', 'lat', 'lon')), may hold values from -1 to 1
- w_proj: bfloat16 [512, 512], P(None, ('mem', 'lat', 'lon')), may hold values from -0.25 to 0.25
- gain_mlp: float32 [512], replicated, may hold values from 0.1 to 1.9
- w_up: bfloat16 [512, 2048], P(None, ('mem', 'lat', 'lon')), may hold values from -0.25 to 0.25
- w_down: bfloat16 [2048, 512], P(None, ('mem', 'lat', 'lon')), may hold values from -0.125 to 0.125
Outputs:
- updated: bfloat16 [4, 2, 96, 96, 512], P('mem', None, 'lat', 'lon')
The draws below stay inside these ranges and needn't reach their ends.
All inputs are finite; a program needn't handle non-finite values.
Results may differ from the reference program's by a relative error of at most 0.011.
Values may be sent and summed in bfloat16 or wider, within the bound.
A program may use at most 192 MiB of HBM per device.

```python
import jax
import jax.numpy as jnp
from jax import lax

D = 512
HEADS = 16
FF = 2048
HDIM = 32
WLAT = 6
WLON = 12
LEVELS = 2
SH = 3
SL = 6
MEMBERS = 4
NLAT = 96
NLON = 96


def draw_w_qkv(key, part):
    first = jax.random.fold_in(key, 11)
    drawn = jnp.clip(jax.random.normal(first, (D, 3 * D), jnp.float32), -6.0, 6.0) / D ** 0.5
    return drawn.astype(jnp.bfloat16)


def with_ends(array, key, least, top_value):
    shape = array.shape
    index_at = [jax.random.randint(jax.random.fold_in(key, axis), (), 0, shape[axis]) for axis in range(len(shape))]
    array = array.at[tuple(index_at)].set(least)
    longest = shape.index(max(shape))
    index_at[longest] = (index_at[longest] + 1) % shape[longest]
    return array.at[tuple(index_at)].set(top_value)


def levels(own_key, dims, split, low, largest):
    factor_of = 1.0
    for axis_at, blocks in split:
        heights = jax.random.uniform(jax.random.fold_in(jax.random.fold_in(own_key, 6), axis_at), (blocks,), jnp.float32, low / len(split), largest / len(split))
        factor_of = factor_of * jnp.repeat(jnp.exp(heights), dims[axis_at] // blocks).reshape((-1,) + (1,) * (len(dims) - 1 - axis_at))
    return factor_of


def scatter_about(rng, dims, deviation, most, split=(), held_as=jnp.bfloat16):
    drawn = deviation * jax.random.normal(rng, dims, jnp.float32)
    if split:
        drawn = drawn * levels(rng, dims, split, -0.22, 0.18)
    return jnp.clip(drawn, -most, most).astype(held_as)


def setup_inputs(seed: int = 0) -> dict:
    splits = jax.random.split(jax.random.key(seed), 9)
    fields = scatter_about(splits[0], (MEMBERS, LEVELS, NLAT, NLON, D), 1.0, 6.0, ((0, 4), (2, 4), (3, 2)))
    region = with_ends(jax.random.randint(splits[1], (NLAT, NLON), 0, 3), jax.random.fold_in(splits[1], 1), 0, 2).astype(jnp.int32)
    gain_attn = jnp.clip(1.0 + 0.18 * jax.random.normal(splits[2], (D,), jnp.float32), 0.1, 1.9)
    w_qkv = draw_w_qkv(jax.random.fold_in(splits[8], 71), 0)
    w_proj = scatter_about(splits[4], (D, D), D ** -0.5, 0.25, ((1, 32),))
    gain_mlp = jnp.clip(1.0 + 0.18 * jax.random.normal(splits[5], (D,), jnp.float32), 0.1, 1.9)
    w_up = scatter_about(splits[6], (D, FF), D ** -0.5, 0.25, ((1, 32),))
    w_down = scatter_about(splits[7], (FF, D), FF ** -0.5, 0.125, ((1, 32),))
    return dict(fields=fields, region=region, gain_attn=gain_attn, w_qkv=w_qkv, w_proj=w_proj, gain_mlp=gain_mlp, w_up=w_up, w_down=w_down)


eps = 1e-05

def layer_norm(values, gain_vec):
    values = values.astype(jnp.float32)
    average = lax.optimization_barrier(jnp.mean(values, axis=-1, keepdims=True))
    centred = values - average
    variance = lax.optimization_barrier(jnp.mean(centred * centred, axis=-1, keepdims=True))
    return (centred * lax.rsqrt(variance + eps) * gain_vec).astype(jnp.bfloat16)

def to_windows(arr):
    chans = arr.shape[-1]
    arr = arr.reshape(LEVELS, NLAT // WLAT, WLAT, NLON // WLON, WLON, chans)
    arr = arr.transpose(1, 3, 0, 2, 4, 5)
    return arr.reshape(NLAT // WLAT, NLON // WLON, LEVELS * WLAT * WLON, chans)

def reference(fields, region, gain_attn, w_qkv, w_proj, gain_mlp, w_up, w_down):
    scale = 1.0 / HDIM ** 0.5
    win_tok = LEVELS * WLAT * WLON
    shifted_ids = jnp.roll(region, (-SH, -SL), axis=(0, 1)).astype(jnp.int32)
    north = ((jnp.arange(NLAT) + SH) % NLAT < SH).astype(jnp.int32)
    ids_win = to_windows(jnp.broadcast_to(shifted_ids[None, :, :, None], (LEVELS, NLAT, NLON, 1)))[..., 0]
    north_win = to_windows(jnp.broadcast_to(north[None, :, None, None], (LEVELS, NLAT, NLON, 1)))[..., 0]

    def band_fn(args):
        tokens, ids_band, north_band = args
        count = tokens.shape[0]
        qkv_all = jnp.dot(tokens.reshape(-1, D), w_qkv, preferred_element_type=jnp.float32).astype(jnp.bfloat16)
        qkv_all = qkv_all.reshape(count, win_tok, 3, HEADS, HDIM).astype(jnp.float32)
        queries = qkv_all[:, :, 0]
        keys_in = qkv_all[:, :, 1]
        values_in = qkv_all[:, :, 2]
        scores = jnp.einsum('wqhd,wkhd->whqk', queries, keys_in) * scale
        allow = (ids_band[:, :, None] == ids_band[:, None, :]) & (north_band[:, :, None] == north_band[:, None, :])
        scores = jnp.where(allow[:, None], scores, -1000000000.0)
        attn_probs = jax.nn.softmax(scores, axis=-1).astype(jnp.bfloat16)
        mixed_heads = jnp.einsum('whqk,wkhd->wqhd', attn_probs.astype(jnp.float32), values_in).astype(jnp.bfloat16)
        mixed_heads = mixed_heads.reshape(count * win_tok, D)
        projected = jnp.dot(mixed_heads, w_proj, preferred_element_type=jnp.float32).astype(jnp.bfloat16)
        return projected.reshape(count, win_tok, D)

    def one_member(member):
        normed = layer_norm(member, gain_attn)
        shifted = jnp.roll(normed, (-SH, -SL), axis=(1, 2))
        out_win = lax.map(band_fn, (to_windows(shifted), ids_win, north_win))
        out_win = out_win.reshape(NLAT // WLAT, NLON // WLON, LEVELS, WLAT, WLON, D)
        attn_out = out_win.transpose(2, 0, 3, 1, 4, 5).reshape(LEVELS, NLAT, NLON, D)
        attn_out = jnp.roll(attn_out, (SH, SL), axis=(1, 2))
        resid = (member.astype(jnp.float32) + attn_out.astype(jnp.float32)).astype(jnp.bfloat16)
        normed2 = layer_norm(resid, gain_mlp).reshape(-1, D)
        hidden = jax.nn.gelu(jnp.dot(normed2, w_up, preferred_element_type=jnp.float32), approximate=False).astype(jnp.bfloat16)
        delta = jnp.dot(hidden, w_down, preferred_element_type=jnp.float32).reshape(LEVELS, NLAT, NLON, D)
        return (resid.astype(jnp.float32) + delta).astype(jnp.bfloat16)
    return lax.map(one_member, fields)
```

```python
import functools

import jax
import jax.numpy as jnp
from jax import lax
from jax.experimental import pallas as pl
from jax.experimental.pallas import tpu as pltpu
from jax.sharding import PartitionSpec as P

HDIM = 32
WLAT = 6
WLON = 12
SH = 3
SL = 6
PAD = 8
LANES = 128
AXES = ("mem", "lat", "lon")
BIG = 1e9
EXP2_SCALE = 1.4426950408889634 / HDIM**0.5

eps = 1e-05

NT = (((1,), (1,)), ((), ()))
TN = (((0,), (0,)), ((), ()))
ALL = slice(None)


def dot32(a, b, dims):
    return lax.dot_general(a, b, dims, preferred_element_type=jnp.float32)


def norm(values, gain):
    average = jnp.mean(values, axis=-1, keepdims=True)
    centred = values - average
    variance = jnp.mean(centred * centred, axis=-1, keepdims=True)
    return (centred * lax.rsqrt(variance + eps) * gain).astype(jnp.bfloat16)


def window_order(bands, wins):
    edge = [(bands - 1, w) for w in range(wins)] + [(b, wins - 1) for b in range(bands - 1)]
    inner = [(b, w) for b in range(bands - 1) for w in range(wins - 1)]
    order = inner[:wins] + edge
    return order + inner[wins:], wins, len(order)


def gather_plan(dims):
    fine = [(d, "lon", "mem") if d % 2 == 0 else (d, "mem", "lon") for d in range(dims["lat"])]
    return [fine, [(None, "lon", "mem")], [(None, "lon", "mem")], [(None, "lon", "mem")]]


def gather_keys(dims):
    keys = []
    for i, parts in enumerate(gather_plan(dims)):
        keys += [("z", i, d) for d in range(1, dims["lat"])]
        for p, (_, a2, a3) in enumerate(parts):
            keys += [("c1", i, p)]
            keys += [(k, i, p, d) for d in range(1, dims[a2]) for k in ("s2", "c2")]
            keys += [(k, i, p, d) for d in range(1, dims[a3]) for k in ("s3", "c3")]
    return keys


HALO = ("rows", "cols", "corner", "id_rows", "id_cols", "id_corner", "back_rows", "back_cols", "back_corner")


class Links:
    def __init__(self, dims, weights, send_sem, recv_sem):
        self.dims = dims
        self.plan = gather_plan(dims)
        self.weights = weights
        self.send_sem = send_sem
        self.recv_sem = recv_sem
        self.slots = {key: n for n, key in enumerate(gather_keys(dims) + list(HALO))}
        mem = lax.axis_index("mem")
        self.core = lax.rem(mem, 2)
        self.at = {"mem": lax.div(mem, 2), "lat": lax.axis_index("lat"), "lon": lax.axis_index("lon")}
        self.partner = {"mem": self.at["mem"] * 2 + 1 - self.core}

    def moved(self, axis, d):
        return lax.rem(self.at[axis] + d + self.dims[axis], self.dims[axis])

    def device(self, **offsets):
        to = {}
        for axis, d in offsets.items():
            position = self.moved(axis, d)
            to[axis] = position * 2 + self.core if axis == "mem" else position
        return to

    def copy(self, key, src, dst, to):
        slot = self.slots[key]
        return pltpu.make_async_remote_copy(
            src_ref=src,
            dst_ref=dst,
            send_sem=self.send_sem.at[slot],
            recv_sem=self.recv_sem.at[slot],
            device_id=to,
            device_id_type=pl.DeviceIdType.MESH,
        )

    def block(self, i, **where):
        index = [where.get(axis, self.at[axis]) for axis in AXES]
        return self.weights[i].at[index[0], self.core, index[1], index[2]]

    def lat_of(self, i, p):
        d = self.plan[i][p][0]
        return ALL if d is None else self.moved("lat", -d)

    def first(self, i, d):
        block = self.block(i)
        return self.copy(("z", i, d), block, block, self.device(lat=d))

    def second(self, i, p, d):
        block = self.block(i, lat=self.lat_of(i, p))
        return self.copy(("s2", i, p, d), block, block, self.device(**{self.plan[i][p][1]: d}))

    def third(self, i, p, d):
        block = self.block(i, lat=self.lat_of(i, p), **{self.plan[i][p][1]: ALL})
        return self.copy(("s3", i, p, d), block, block, self.device(**{self.plan[i][p][2]: d}))

    def cross(self, stage, i, p, d=None):
        _, a2, a3 = self.plan[i][p]
        where = {"lat": self.lat_of(i, p)}
        if stage == 2:
            where[a2] = self.moved(a2, -d)
        if stage == 3:
            where[a2] = ALL
            where[a3] = self.moved(a3, -d)
        block = self.block(i, **where)
        key = ("c1", i, p) if stage == 1 else ("c%d" % stage, i, p, d)
        return self.copy(key, block, block, self.partner)

    def peers(self, axis):
        return range(1, self.dims[axis])

    def start_first(self, i):
        for d in self.peers("lat"):
            self.first(i, d).start()

    def to_second(self, i, p):
        lat, a2, _ = self.plan[i][p]
        for d in self.peers("lat"):
            if lat in (None, d):
                self.first(i, d).wait_recv()
        for d in self.peers(a2):
            self.second(i, p, d).start()
        self.cross(1, i, p).start()

    def to_third(self, i, p):
        _, a2, a3 = self.plan[i][p]
        for d in self.peers(a2):
            self.second(i, p, d).wait_recv()
        for d in self.peers(a3):
            self.third(i, p, d).start()
        for d in self.peers(a2):
            self.cross(2, i, p, d).start()

    def to_cross(self, i, p):
        for d in self.peers(self.plan[i][p][2]):
            self.third(i, p, d).wait_recv()
            self.cross(3, i, p, d).start()

    def crossings(self, i, p):
        _, a2, a3 = self.plan[i][p]
        yield self.cross(1, i, p)
        for d in self.peers(a2):
            yield self.cross(2, i, p, d)
        for d in self.peers(a3):
            yield self.cross(3, i, p, d)

    def arrive(self, i):
        for p in range(len(self.plan[i])):
            for copy in self.crossings(i, p):
                copy.wait_recv()

    def drain(self, i):
        for d in self.peers("lat"):
            self.first(i, d).wait_send()
        for p, (_, a2, a3) in enumerate(self.plan[i]):
            for d in self.peers(a2):
                self.second(i, p, d).wait_send()
            for d in self.peers(a3):
                self.third(i, p, d).wait_send()
            for copy in self.crossings(i, p):
                copy.wait_send()

    def greet(self):
        barrier = pltpu.get_barrier_semaphore()
        others = [self.partner]
        for axis in AXES:
            others += [self.device(**{axis: d}) for d in self.peers(axis)]
        others += [self.device(lat=1, lon=1), self.device(lat=-1, lon=-1)]
        for to in others:
            pl.semaphore_signal(barrier, inc=1, device_id=to, device_id_type=pl.DeviceIdType.MESH)
        pl.semaphore_wait(barrier, len(others))


def attention_kernel(
    dims,
    x_ref,
    hot_ref,
    gain_ref,
    wqkv_ref,
    wproj_ref,
    wup_ref,
    wdown_ref,
    resid_ref,
    cols_ref,
    up_ref,
    down_ref,
    ext_s,
    hotx_s,
    grid_s,
    hotg_s,
    tok_s,
    hot_s,
    normed_s,
    qkv_s,
    mix_s,
    wqkv_s,
    wproj_s,
    own_sem,
    send_sem,
    recv_sem,
):
    levels, clat, clon, width = x_ref.shape
    bands, wins = clat // WLAT, clon // WLON
    wtok = levels * WLAT * WLON
    order, early, late = window_order(bands, wins)
    count = len(order)
    groups = count // wins
    gtok = wins * wtok

    links = Links(dims, [wqkv_s, wproj_s, up_ref, down_ref], send_sem, recv_sem)
    own = [
        pltpu.make_async_copy(shard, links.block(i), own_sem.at[i])
        for i, shard in enumerate([wqkv_ref, wproj_ref, wup_ref, wdown_ref])
    ]
    own.append(pltpu.make_async_copy(x_ref, ext_s.at[:, pl.ds(0, clat), pl.ds(0, clon)], own_sem.at[4]))
    own.append(pltpu.make_async_copy(hot_ref, hotx_s.at[pl.ds(0, clat), pl.ds(0, clon)], own_sem.at[5]))
    for copy in own:
        copy.start()

    top, side = pl.ds(0, SH), pl.ds(0, PAD)
    body_rows, body_cols = pl.ds(0, clat), pl.ds(0, clon)
    below, beyond = pl.ds(clat, SH), pl.ds(clon, PAD)
    lat_prev, lon_prev, prev = links.device(lat=-1), links.device(lon=-1), links.device(lat=-1, lon=-1)
    rows_in = [
        links.copy("rows", x_ref.at[:, top], ext_s.at[:, below, body_cols], lat_prev),
        links.copy("id_rows", hot_ref.at[top], hotx_s.at[below, body_cols], lat_prev),
    ]
    cols_in = [
        links.copy("cols", x_ref.at[:, :, side], ext_s.at[:, body_rows, beyond], lon_prev),
        links.copy("id_cols", hot_ref.at[:, side], hotx_s.at[body_rows, beyond], lon_prev),
        links.copy("corner", x_ref.at[:, top, side], ext_s.at[:, below, beyond], prev),
        links.copy("id_corner", hot_ref.at[top, side], hotx_s.at[below, beyond], prev),
    ]

    links.greet()
    own[0].wait()
    links.start_first(0)
    links.to_second(0, 0)
    for copy in rows_in:
        copy.start()
    for i in range(1, 4):
        own[i].wait()
        links.start_first(i)
    for copy in own[4:]:
        copy.wait()

    def widen(rows, cols):
        def row(r, _):
            for l in range(levels):
                grid_s[l, r, cols, :] = ext_s[l, r, cols, :].astype(jnp.float32)
            hotg_s[r, cols, :] = hotx_s[r, cols, :].astype(jnp.float32)
            return 0

        lax.fori_loop(rows[0], rows[1], row, 0)

    def fetch(slot):
        b, w = order[slot]
        for r in range(WLAT):
            cols = pl.ds(SL + w * WLON, WLON)
            for l in range(levels):
                to = pl.ds(slot * wtok + (l * WLAT + r) * WLON, WLON)
                tok_s[to, :] = grid_s[l, SH + b * WLAT + r, cols, :]
                hot_s[to, :] = hotg_s[SH + b * WLAT + r, cols, :]

    def norms(first, last):
        def one(s, _):
            rows = pl.ds(pl.multiple_of(s * wtok, wtok), wtok)
            normed_s[rows, :] = norm(tok_s[rows, :], gain_ref[...])
            return 0

        lax.fori_loop(first, last, one, 0)

    fine = len(links.plan[0])
    widen((0, clat), pl.ds(0, clon))
    for p in range(1, fine):
        links.to_second(0, p)
    links.to_third(0, 0)
    for copy in cols_in:
        copy.start()
    for slot in list(range(early)) + list(range(late, count)):
        fetch(slot)
    for p in range(1, fine):
        links.to_third(0, p)
    norms(0, early)
    norms(late, count)
    for p in range(fine):
        links.to_cross(0, p)
    links.to_second(1, 0)
    for copy in rows_in + cols_in:
        copy.wait_recv()
    widen((0, clat), pl.ds(clon, PAD))
    widen((clat, clat + SH), pl.ds(0, clon + PAD))
    for slot in range(early, late):
        fetch(slot)
    norms(early, late)
    links.arrive(0)

    wqkv = wqkv_s[...].reshape(3 * width, width)
    per = LANES // HDIM
    lane_head = lax.broadcasted_iota(jnp.int32, (wtok, LANES), 1) // HDIM

    def pump(step):
        moves = {
            1: lambda: links.to_third(1, 0),
            3: lambda: links.to_second(2, 0),
            wins - 1 + wins: lambda: links.to_second(3, 0),
            wins + wins: lambda: links.to_third(2, 0),
            3 * wins: lambda: links.to_third(3, 0),
        }
        for at, move in moves.items():
            pl.when(step == at)(move)

    def out_piece(slot):
        b, w = order[slot]
        for l in range(levels):
            for r in range(WLAT):
                t = pl.ds(slot * wtok + (l * WLAT + r) * WLON, WLON)
                grid_s[l, SH + b * WLAT + r, pl.ds(SL + w * WLON, WLON), :] = tok_s[t, :]

    def narrow(rows, cols):
        def row(r, _):
            for l in range(levels):
                ext_s[l, r, cols, :] = grid_s[l, r, cols, :].astype(jnp.bfloat16)
            return 0

        lax.fori_loop(rows[0], rows[1], row, 0)

    lat_next, lon_next, following = links.device(lat=1), links.device(lon=1), links.device(lat=1, lon=1)
    lower = pl.ds(SH, clat - SH)
    back = [
        links.copy("back_rows", ext_s.at[:, below, body_cols], resid_ref.at[:, top], lat_next),
        links.copy("back_cols", ext_s.at[:, lower, beyond], cols_ref.at[:, lower], lon_next),
        links.copy("back_corner", ext_s.at[:, below, beyond], cols_ref.at[:, top], following),
    ]

    def group(g, _):
        base = pl.multiple_of(g * gtok, gtok)
        mine = pl.ds(base, gtok)
        for part in range(3):
            at = pl.ds(part * width, width)
            qkv_s[:, at] = dot32(normed_s[mine, :], wqkv[part * width : (part + 1) * width], NT).astype(jnp.bfloat16)

        def window(w, _):
            pump(g * wins + w)
            rows = pl.ds(pl.multiple_of(w * wtok, wtok), wtok)
            hot = hot_s[pl.ds(pl.multiple_of(base + w * wtok, wtok), wtok), :].astype(jnp.bfloat16)
            barred = ((hot.astype(jnp.float32) - 1.0) * BIG).astype(jnp.bfloat16)
            for h4 in range(width // LANES):
                q = qkv_s[rows, pl.ds(h4 * LANES, LANES)]
                k = qkv_s[rows, pl.ds(width + h4 * LANES, LANES)]
                v = qkv_s[rows, pl.ds(2 * width + h4 * LANES, LANES)]
                queries = jnp.concatenate(
                    [
                        jnp.concatenate([jnp.where(lane_head == h, q, jnp.zeros_like(q)), hot], axis=1)
                        for h in range(per)
                    ],
                    axis=0,
                )
                keys = jnp.concatenate([k, barred], axis=1)
                scores = dot32(keys, queries, NT)
                most = jnp.max(scores, axis=0, keepdims=True)
                probs = jnp.exp2((scores - most) * EXP2_SCALE)
                total = jnp.sum(probs, axis=0, keepdims=True)
                mixed = dot32(v, probs.astype(jnp.bfloat16), TN) * (1.0 / total)
                heads = [mixed[h * HDIM : (h + 1) * HDIM, h * wtok : (h + 1) * wtok] for h in range(per)]
                mix_s[rows, pl.ds(h4 * LANES, LANES)] = jnp.concatenate(heads, axis=0).T.astype(jnp.bfloat16)
            return 0

        lax.fori_loop(0, wins, window, 0)

        @pl.when(g == 0)
        def _():
            links.to_cross(1, 0)
            links.arrive(1)

        wproj = wproj_s[...].reshape(width, width)
        attn_out = dot32(mix_s[...], wproj, NT).astype(jnp.bfloat16).astype(jnp.float32)
        tok_s[mine, :] += attn_out

        @pl.when(g == (late - 1) // wins)
        def _():
            for slot in range(early, late):
                out_piece(slot)
            narrow((clat, clat + SH), pl.ds(0, clon + PAD))
            narrow((SH, clat), pl.ds(clon, PAD))
            for copy in back:
                copy.start()

        return 0

    lax.fori_loop(0, groups, group, 0)
    for slot in list(range(early)) + list(range(late, count)):
        out_piece(slot)
    narrow((SH, clat), pl.ds(0, clon))
    keep = pltpu.make_async_copy(ext_s.at[:, lower, body_cols], resid_ref.at[:, lower], own_sem.at[0])
    keep.start()
    for i in (2, 3):
        links.to_cross(i, 0)
    for copy in rows_in + cols_in:
        copy.wait_send()
    for i in (0, 1):
        links.drain(i)
    for i in (2, 3):
        links.arrive(i)
        links.drain(i)
    for copy in back:
        copy.wait()
    keep.wait()


def attention(member, hot, gain, shards):
    dims = {"mem": lax.axis_size("mem") // 2, "lat": lax.axis_size("lat"), "lon": lax.axis_size("lon")}
    lead = (dims["mem"], 2, dims["lat"], dims["lon"])
    levels, clat, clon, width = member.shape
    bands, wins = clat // WLAT, clon // WLON
    ntok = levels * clat * clon
    gtok = ntok // bands
    slots = len(gather_keys(dims)) + len(HALO)
    anywhere = pl.BlockSpec(memory_space=pl.ANY)
    ext = (levels, clat + SH, clon + PAD, width)
    hot_ext = (clat + SH, clon + PAD, LANES)
    whole = [lead + s.shape for s in shards]
    outs = pl.pallas_call(
        functools.partial(attention_kernel, dims),
        out_shape=[
            jax.ShapeDtypeStruct(member.shape, jnp.bfloat16),
            jax.ShapeDtypeStruct((levels, clat, PAD, width), jnp.bfloat16),
            jax.ShapeDtypeStruct(whole[2], jnp.bfloat16),
            jax.ShapeDtypeStruct(whole[3], jnp.bfloat16),
        ],
        in_specs=[anywhere, anywhere, pl.BlockSpec(memory_space=pltpu.VMEM)] + [anywhere] * 4,
        out_specs=[anywhere] * 4,
        scratch_shapes=[
            pltpu.VMEM(ext, jnp.bfloat16),
            pltpu.VMEM(hot_ext, jnp.bfloat16),
            pltpu.VMEM(ext, jnp.float32),
            pltpu.VMEM(hot_ext, jnp.float32),
            pltpu.VMEM((ntok, width), jnp.float32),
            pltpu.VMEM((ntok, LANES), jnp.float32),
            pltpu.VMEM((ntok, width), jnp.bfloat16),
            pltpu.VMEM((gtok, 3 * width), jnp.bfloat16),
            pltpu.VMEM((gtok, width), jnp.bfloat16),
            pltpu.VMEM(whole[0], jnp.bfloat16),
            pltpu.VMEM(whole[1], jnp.bfloat16),
            pltpu.SemaphoreType.DMA((6,)),
            pltpu.SemaphoreType.DMA((slots,)),
            pltpu.SemaphoreType.DMA((slots,)),
        ],
        compiler_params=pltpu.CompilerParams(
            collective_id=0, has_side_effects=True, vmem_limit_bytes=56 * 2**20
        ),
        cost_estimate=pl.CostEstimate(
            flops=8 * ntok * width * width, bytes_accessed=4 * ntok * width, transcendentals=ntok * 4096
        ),
    )(member, hot, gain, *shards)
    return outs[0], outs[1], outs[2].reshape(-1, width), outs[3].reshape(width, -1)


def mlp_kernel(resid_ref, cols_ref, gain_ref, wup_ref, wdown_ref, out_ref, acc_s):
    levels, rows, cols, width = out_ref.shape
    hidden_all = wup_ref.shape[0]
    block = resid_ref[...].astype(jnp.float32)
    came = cols_ref[...].astype(jnp.float32)
    ours = lax.broadcasted_iota(jnp.int32, came.shape, 2) >= SL
    edge = jnp.where(ours, block[:, :, :PAD], came)
    resid = jnp.concatenate([edge, block[:, :, PAD:]], axis=2).reshape(levels * rows * cols, width)
    normed = norm(resid, gain_ref[...])
    acc_s[...] = resid
    step = min(width, hidden_all)
    for at in range(0, hidden_all, step):
        pre = dot32(normed, wup_ref[pl.ds(at, step), :], NT)
        hidden = (0.5 * pre * (1.0 + lax.erf(pre * 0.5**0.5))).astype(jnp.bfloat16)
        acc_s[...] += dot32(hidden, wdown_ref[:, pl.ds(at, step)], NT)
    out_ref[...] = acc_s[...].reshape(out_ref.shape).astype(jnp.bfloat16)


def whole(shape):
    return pl.BlockSpec(shape, lambda b: (0,) * len(shape))


def body(fields, region, gain_attn, w_qkv, w_proj, gain_mlp, w_up, w_down):
    member = fields[0]
    levels, clat, clon, width = member.shape
    bands = clat // WLAT
    count = levels * clat * clon

    north = (lax.axis_index("lat") * clat + jnp.arange(clat, dtype=jnp.int32)) < SH
    ids = region.astype(jnp.int32) + 3 * north[:, None].astype(jnp.int32)
    hot = (ids[:, :, None] == jnp.arange(LANES, dtype=jnp.int32)).astype(jnp.bfloat16)

    resid, came, wup_t, wdown_t = attention(
        member, hot, gain_attn[None], [w_qkv.T, w_proj.T, w_up.T, w_down.T]
    )

    grid_block = pl.BlockSpec((levels, WLAT, clon, width), lambda b: (0, b, 0, 0))
    came_block = pl.BlockSpec((levels, WLAT, PAD, width), lambda b: (0, b, 0, 0))
    out = pl.pallas_call(
        mlp_kernel,
        grid=(bands,),
        in_specs=[grid_block, came_block, whole((1, width)), whole(wup_t.shape), whole(wdown_t.shape)],
        out_specs=grid_block,
        out_shape=jax.ShapeDtypeStruct(member.shape, jnp.bfloat16),
        scratch_shapes=[pltpu.VMEM((count // bands, width), jnp.float32)],
        compiler_params=pltpu.CompilerParams(dimension_semantics=("arbitrary",), vmem_limit_bytes=56 * 2**20),
        cost_estimate=pl.CostEstimate(
            flops=4 * count * width * wup_t.shape[0], bytes_accessed=4 * count * width, transcendentals=count * 2048
        ),
    )(resid, came, gain_mlp[None], wup_t, wdown_t)
    return out[None]


def solution(mesh):
    columns = P(None, AXES)
    in_specs = (P("mem", None, "lat", "lon", None), P("lat", "lon"), P(), columns, columns, P(), columns, columns)
    out_specs = P("mem", None, "lat", "lon", None)
    return jax.shard_map(body, mesh=mesh, in_specs=in_specs, out_specs=out_specs, check_vma=False)
```

```python
import functools

import jax
import jax.numpy as jnp
from jax import lax
from jax.experimental import pallas as pl
from jax.experimental.pallas import tpu as pltpu
from jax.sharding import PartitionSpec as P

HDIM = 32
WLAT = 6
WLON = 12
SH = 3
SL = 6
PAD = 8
LANES = 128
AXES = ("mem", "lat", "lon")
BIG = 1e9
EXP2_SCALE = 1.4426950408889634 / HDIM**0.5

eps = 1e-05

NT = (((1,), (1,)), ((), ()))
TN = (((0,), (0,)), ((), ()))
ALL = slice(None)


def dot32(a, b, dims):
    return lax.dot_general(a, b, dims, preferred_element_type=jnp.float32)


def norm(values, gain):
    average = jnp.mean(values, axis=-1, keepdims=True)
    centred = values - average
    variance = jnp.mean(centred * centred, axis=-1, keepdims=True)
    return (centred * lax.rsqrt(variance + eps) * gain).astype(jnp.bfloat16)


def window_order(bands, wins):
    rows = [(bands - 1, w) for w in range(wins - 1)]
    cols = [(b, wins - 1) for b in range(bands)]
    inner = [(b, w) for b in range(bands - 1) for w in range(wins - 1)]
    order, inner = inner[:wins], inner[wins:]
    marks = []
    for edge in (rows, cols):
        fill = -len(edge) % wins
        marks.append((len(order), len(order) + len(edge)))
        order, inner = order + edge + inner[:fill], inner[fill:]
    return order + inner, marks[0], marks[1]


def gather_plan(dims):
    last, middle = dims["lat"] - 1, dims["lat"] // 2
    ways = ("lon", "mem"), ("mem", "lon")
    fine = [(d,) + ways[d == last] for d in range(dims["lat"])]
    up = [(d,) + ways[d == middle] for d in range(dims["lat"])]
    down = [(d,) + ways[0] for d in range(dims["lat"])]
    return [fine, [(None,) + ways[0]], up, down]


def gather_keys(dims):
    keys = []
    for i, parts in enumerate(gather_plan(dims)):
        keys += [("z", i, d) for d in range(1, dims["lat"])]
        for p, (_, a2, a3) in enumerate(parts):
            keys += [("c1", i, p)]
            keys += [(k, i, p, d) for d in range(1, dims[a2]) for k in ("s2", "c2")]
            keys += [(k, i, p, d) for d in range(1, dims[a3]) for k in ("s3", "c3")]
    return keys


HALO = ("rows", "cols", "corner", "id_rows", "id_cols", "id_corner", "back_rows", "back_cols", "back_corner")
STAGES = 4


class Links:
    def __init__(self, dims, weights, send_sem, recv_sem):
        self.dims = dims
        self.plan = gather_plan(dims)
        self.weights = weights
        self.send_sem = send_sem
        self.recv_sem = recv_sem
        self.slots = {key: n for n, key in enumerate(gather_keys(dims) + list(HALO))}
        mem = lax.axis_index("mem")
        self.core = lax.rem(mem, 2)
        self.at = {"mem": lax.div(mem, 2), "lat": lax.axis_index("lat"), "lon": lax.axis_index("lon")}
        self.partner = {"mem": self.at["mem"] * 2 + 1 - self.core}

    def moved(self, axis, d):
        return lax.rem(self.at[axis] + d + self.dims[axis], self.dims[axis])

    def device(self, **offsets):
        to = {}
        for axis, d in offsets.items():
            position = self.moved(axis, d)
            to[axis] = position * 2 + self.core if axis == "mem" else position
        return to

    def copy(self, key, src, dst, to):
        slot = self.slots[key]
        return pltpu.make_async_remote_copy(
            src_ref=src,
            dst_ref=dst,
            send_sem=self.send_sem.at[slot],
            recv_sem=self.recv_sem.at[slot],
            device_id=to,
            device_id_type=pl.DeviceIdType.MESH,
        )

    def block(self, i, **where):
        index = [where.get(axis, self.at[axis]) for axis in AXES]
        return self.weights[i].at[index[0], self.core, index[1], index[2]]

    def lat_of(self, i, p):
        d = self.plan[i][p][0]
        return ALL if d is None else self.moved("lat", -d)

    def first(self, i, d):
        block = self.block(i)
        return self.copy(("z", i, d), block, block, self.device(lat=d))

    def second(self, i, p, d):
        block = self.block(i, lat=self.lat_of(i, p))
        return self.copy(("s2", i, p, d), block, block, self.device(**{self.plan[i][p][1]: d}))

    def third(self, i, p, d):
        block = self.block(i, lat=self.lat_of(i, p), **{self.plan[i][p][1]: ALL})
        return self.copy(("s3", i, p, d), block, block, self.device(**{self.plan[i][p][2]: d}))

    def cross(self, stage, i, p, d=None):
        _, a2, a3 = self.plan[i][p]
        where = {"lat": self.lat_of(i, p)}
        if stage == 2:
            where[a2] = self.moved(a2, -d)
        if stage == 3:
            where[a2] = ALL
            where[a3] = self.moved(a3, -d)
        block = self.block(i, **where)
        key = ("c1", i, p) if stage == 1 else ("c%d" % stage, i, p, d)
        return self.copy(key, block, block, self.partner)

    def peers(self, axis):
        return range(1, self.dims[axis])

    def start_first(self, i):
        for d in self.near():
            self.first(i, d).start()

    def near(self):
        n = self.dims["lat"]
        return sorted(self.peers("lat"), key=lambda d: min(d, n - d))

    def to_second(self, i, p):
        lat, a2, _ = self.plan[i][p]
        for d in self.peers("lat"):
            if lat in (None, d):
                self.first(i, d).wait_recv()
        for d in self.peers(a2):
            self.second(i, p, d).start()
        self.cross(1, i, p).start()

    def to_third(self, i, p):
        _, a2, a3 = self.plan[i][p]
        for d in self.peers(a2):
            self.second(i, p, d).wait_recv()
        for d in self.peers(a3):
            self.third(i, p, d).start()
        for d in self.peers(a2):
            self.cross(2, i, p, d).start()

    def to_cross(self, i, p):
        for d in self.peers(self.plan[i][p][2]):
            self.third(i, p, d).wait_recv()
            self.cross(3, i, p, d).start()

    def crossings(self, i, p):
        _, a2, a3 = self.plan[i][p]
        yield self.cross(1, i, p)
        for d in self.peers(a2):
            yield self.cross(2, i, p, d)
        for d in self.peers(a3):
            yield self.cross(3, i, p, d)

    def arrive(self, i):
        for p in range(len(self.plan[i])):
            for copy in self.crossings(i, p):
                copy.wait_recv()

    def drain(self, i):
        for d in self.peers("lat"):
            self.first(i, d).wait_send()
        for p, (_, a2, a3) in enumerate(self.plan[i]):
            for d in self.peers(a2):
                self.second(i, p, d).wait_send()
            for d in self.peers(a3):
                self.third(i, p, d).wait_send()
            for copy in self.crossings(i, p):
                copy.wait_send()

    def greet(self):
        barrier = pltpu.get_barrier_semaphore()
        others = [self.partner]
        for axis in AXES:
            others += [self.device(**{axis: d}) for d in self.peers(axis)]
        others += [self.device(lat=1, lon=1), self.device(lat=-1, lon=-1)]
        for to in others:
            pl.semaphore_signal(barrier, inc=1, device_id=to, device_id_type=pl.DeviceIdType.MESH)
        pl.semaphore_wait(barrier, len(others))


def attention_kernel(
    dims,
    x_ref,
    region_ref,
    gain_ref,
    wqkv_ref,
    wproj_ref,
    wup_ref,
    wdown_ref,
    resid_ref,
    cols_ref,
    up_ref,
    down_ref,
    ext_s,
    ids_s,
    grid_s,
    hotg_s,
    tok_s,
    hot_s,
    normed_s,
    qkv_s,
    mix_s,
    score_s,
    prob_s,
    wqkv_s,
    wproj_s,
    own_sem,
    send_sem,
    recv_sem,
):
    levels, clat, clon, width = x_ref.shape
    bands, wins = clat // WLAT, clon // WLON
    wtok = levels * WLAT * WLON
    order, (row_first, row_last), (col_first, col_last) = window_order(bands, wins)
    count = len(order)
    groups = count // wins
    gtok = wins * wtok
    chunks = dims["lat"]
    edge = list(range(row_first, row_last)) + list(range(col_first, col_last))

    links = Links(dims, [wqkv_s, wproj_s, up_ref, down_ref], send_sem, recv_sem)
    own = [
        pltpu.make_async_copy(shard, links.block(i), own_sem.at[i])
        for i, shard in enumerate([wqkv_ref, wproj_ref, wup_ref, wdown_ref])
    ]
    own.append(pltpu.make_async_copy(x_ref, ext_s.at[:, pl.ds(0, clat), pl.ds(0, clon)], own_sem.at[4]))
    for copy in own:
        copy.start()

    north = lax.broadcasted_iota(jnp.int32, (clat, clon), 0) + lax.axis_index("lat") * clat < SH
    ids_s[0] = jnp.zeros((clat, LANES), jnp.float32)
    ids_s[0, :, pl.ds(0, clon)] = (region_ref[...] + jnp.where(north, 3, 0)).astype(jnp.float32)

    top, side = pl.ds(0, SH), pl.ds(0, PAD)
    body_rows, body_cols = pl.ds(0, clat), pl.ds(0, clon)
    below, beyond = pl.ds(clat, SH), pl.ds(clon, PAD)
    lat_prev, lon_prev, prev = links.device(lat=-1), links.device(lon=-1), links.device(lat=-1, lon=-1)
    ids_in = [
        links.copy("id_rows", ids_s.at[0], ids_s.at[1], lat_prev),
        links.copy("id_cols", ids_s.at[0], ids_s.at[2], lon_prev),
        links.copy("id_corner", ids_s.at[0], ids_s.at[3], prev),
    ]
    rows_in = [links.copy("rows", x_ref.at[:, top], ext_s.at[:, below, body_cols], lat_prev)]
    cols_in = [
        links.copy("cols", x_ref.at[:, :, side], ext_s.at[:, body_rows, beyond], lon_prev),
        links.copy("corner", x_ref.at[:, top, side], ext_s.at[:, below, beyond], prev),
    ]

    links.greet()
    own[0].wait()
    links.start_first(0)
    links.to_second(0, 0)
    for copy in own[1:]:
        copy.wait()

    def widen(rows, cols):
        def row(r, _):
            for l in range(levels):
                grid_s[l, r, cols, :] = ext_s[l, r, cols, :].astype(jnp.float32)
            return 0

        lax.fori_loop(rows[0], rows[1], row, 0)

    def one_hot(planes, rows, cols):
        turned = planes.T
        lane = lax.broadcasted_iota(jnp.int32, (cols, LANES), 1).astype(jnp.float32)
        for r in range(rows[1] - rows[0]):
            hotg_s[rows[0] + r, pl.ds(0, cols), :] = jnp.where(turned[:cols, r : r + 1] == lane, 1.0, 0.0)

    def joined(here, there):
        lane = lax.broadcasted_iota(jnp.int32, here.shape, 1)
        return jnp.where(lane < clon, here, pltpu.roll(there, clon, 1))

    def fetch(slot):
        b, w = order[slot]
        for r in range(WLAT):
            cols = pl.ds(SL + w * WLON, WLON)
            for l in range(levels):
                to = pl.ds(slot * wtok + (l * WLAT + r) * WLON, WLON)
                tok_s[to, :] = grid_s[l, SH + b * WLAT + r, cols, :]
                hot_s[to, :] = hotg_s[SH + b * WLAT + r, cols, :]

    def norms(first, last):
        def one(s, _):
            rows = pl.ds(pl.multiple_of(s * wtok, wtok), wtok)
            normed_s[rows, :] = norm(tok_s[rows, :], gain_ref[...])
            return 0

        lax.fori_loop(first, last, one, 0)

    near = links.near()
    half = wins // 2
    widen((0, clat), pl.ds(0, clon))
    links.to_second(0, near[0])
    links.to_third(0, 0)
    links.start_first(1)
    one_hot(ids_s[0], (0, clat), clon)
    for slot in range(half):
        fetch(slot)
    for p in near[1:]:
        links.to_second(0, p)
    links.start_first(2)
    links.to_second(2, 0)
    for slot in range(half, wins):
        fetch(slot)
    for p in near:
        links.to_third(0, p)
    for copy in rows_in + ids_in:
        copy.start()
    links.start_first(3)
    links.to_second(1, 0)
    links.to_third(2, 0)
    norms(0, wins)
    for slot in range(row_last, count):
        if slot not in edge:
            fetch(slot)
    norms(row_last, col_first)
    norms(col_last, count)
    for p in [0] + near:
        links.to_cross(0, p)
    links.to_second(3, 0)
    links.to_second(2, near[0])
    links.arrive(0)

    def fetch_rows():
        for copy in ids_in + rows_in:
            copy.wait_recv()
        widen((clat, clat + SH), pl.ds(0, clon))
        one_hot(joined(ids_s[0], ids_s[2]), (0, clat), clon + PAD)
        one_hot(joined(ids_s[1, :PAD], ids_s[3, :PAD]), (clat, clat + SH), clon + PAD)
        for slot in range(row_first, row_last):
            fetch(slot)
        norms(row_first, row_last)

    def fetch_cols():
        for copy in cols_in:
            copy.wait_recv()
        widen((0, clat + SH), pl.ds(clon, PAD))
        for slot in range(col_first, col_last):
            fetch(slot)
        norms(col_first, col_last)

    wqkv = wqkv_s[...].reshape(3 * width, width)
    per = LANES // HDIM
    fours = width // LANES
    per_step = 2 if wins % 2 == 0 else 1
    lane_head = lax.broadcasted_iota(jnp.int32, (wtok, LANES), 1) // HDIM

    moves = {}

    def at_step(step, *move):
        moves.setdefault(step, []).append(move)

    def start_cols():
        for copy in cols_in:
            copy.start()

    at_step(0, start_cols)
    at_step(0, links.to_third, 1, 0)
    for n, p in enumerate(near[1:]):
        at_step(2 * n + 1, links.to_second, 2, p)
    for n, p in enumerate(near):
        at_step(3 + n, links.to_third, 2, p)
    for n, p in enumerate(near):
        at_step(3 + n, links.to_second, 3, p)
    at_step(4, links.to_third, 3, 0)
    for n, p in enumerate(near):
        at_step(5 + n, links.to_third, 3, p)
    for p in range(chunks):
        at_step(7, links.to_cross, 2, p)

    def pump(step):
        for at, todo in moves.items():

            @pl.when(step == at)
            def _():
                for move, *where in todo:
                    move(*where)

    def out_piece(slot):
        b, w = order[slot]
        for l in range(levels):
            for r in range(WLAT):
                t = pl.ds(slot * wtok + (l * WLAT + r) * WLON, WLON)
                grid_s[l, SH + b * WLAT + r, pl.ds(SL + w * WLON, WLON), :] = tok_s[t, :]

    def narrow(rows, cols):
        def row(r, _):
            for l in range(levels):
                ext_s[l, r, cols, :] = grid_s[l, r, cols, :].astype(jnp.bfloat16)
            return 0

        lax.fori_loop(rows[0], rows[1], row, 0)

    lat_next, lon_next, following = links.device(lat=1), links.device(lon=1), links.device(lat=1, lon=1)
    lower = pl.ds(SH, clat - SH)
    back = [
        links.copy("back_rows", ext_s.at[:, below, body_cols], resid_ref.at[:, top], lat_next),
        links.copy("back_cols", ext_s.at[:, lower, beyond], cols_ref.at[:, lower], lon_next),
        links.copy("back_corner", ext_s.at[:, below, beyond], cols_ref.at[:, top], following),
    ]

    def group(g, _):
        base = pl.multiple_of(g * gtok, gtok)
        mine = pl.ds(base, gtok)
        pl.when(g == row_first // wins)(fetch_rows)
        pl.when(g == col_first // wins)(fetch_cols)
        for part in range(3):
            at = pl.ds(part * width, width)
            qkv_s[:, at] = dot32(normed_s[mine, :], wqkv[part * width : (part + 1) * width], NT).astype(jnp.bfloat16)

        def windows(u, _):
            pump(g * (wins // per_step) + u)
            rows = [pl.ds(pl.multiple_of((u * per_step + j) * wtok, wtok), wtok) for j in range(per_step)]
            hots = []
            for j in range(per_step):
                at = pl.multiple_of(base + (u * per_step + j) * wtok, wtok)
                hot = hot_s[pl.ds(at, wtok), :].astype(jnp.bfloat16)
                hots.append((hot, ((hot.astype(jnp.float32) - 1.0) * BIG).astype(jnp.bfloat16)))

            def score(i):
                j, f = divmod(i, fours)
                hot, barred = hots[j]
                q = qkv_s[rows[j], pl.ds(f * LANES, LANES)]
                k = qkv_s[rows[j], pl.ds(width + f * LANES, LANES)]
                queries = [jnp.concatenate([jnp.where(lane_head == h, q, jnp.zeros_like(q)), hot], axis=1) for h in range(per)]
                score_s[i % STAGES] = dot32(jnp.concatenate([k, barred], axis=1), jnp.concatenate(queries, axis=0), NT)

            def soften(i):
                scores = score_s[i % STAGES]
                most = jnp.max(scores, axis=0, keepdims=True)
                prob_s[i % STAGES] = jnp.exp2((scores - most) * EXP2_SCALE).astype(jnp.bfloat16)

            def mix(i):
                j, f = divmod(i, fours)
                v = qkv_s[rows[j], pl.ds(2 * width + f * LANES, LANES)]
                ones = jnp.ones((wtok, HDIM // 2), jnp.bfloat16)
                mixed = dot32(jnp.concatenate([v, ones], axis=1), prob_s[i % STAGES], TN)
                heads = []
                for h in range(per):
                    at = slice(h * wtok, (h + 1) * wtok)
                    heads.append(mixed[h * HDIM : (h + 1) * HDIM, at] * (1.0 / mixed[LANES : LANES + 1, at]))
                mix_s[rows[j], pl.ds(f * LANES, LANES)] = jnp.concatenate(heads, axis=0).astype(jnp.bfloat16).T

            items = per_step * fours
            for t in range(items + 3):
                if t < items:
                    score(t)
                if 0 <= t - 2 < items:
                    soften(t - 2)
                if 0 <= t - 3 < items:
                    mix(t - 3)
            return 0

        lax.fori_loop(0, wins // per_step, windows, 0)

        @pl.when(g == 0)
        def _():
            links.to_cross(1, 0)
            links.arrive(1)

        wproj = wproj_s[...].reshape(width, width)
        attn_out = dot32(mix_s[...], wproj, NT).astype(jnp.bfloat16).astype(jnp.float32)
        tok_s[mine, :] += attn_out

        @pl.when(g == (col_last - 1) // wins)
        def _():
            for slot in edge:
                out_piece(slot)
            narrow((clat, clat + SH), pl.ds(0, clon + PAD))
            narrow((SH, clat), pl.ds(clon, PAD))
            for copy in back:
                copy.start()

        return 0

    lax.fori_loop(0, groups, group, 0)
    for slot in range(count):
        if slot not in edge:
            out_piece(slot)
    narrow((SH, clat), pl.ds(0, clon))
    keep = pltpu.make_async_copy(ext_s.at[:, lower, body_cols], resid_ref.at[:, lower], own_sem.at[0])
    keep.start()
    for p in range(chunks):
        links.to_cross(3, p)
    for copy in ids_in + rows_in + cols_in:
        copy.wait_send()
    for i in (0, 1):
        links.drain(i)
    for i in (2, 3):
        links.arrive(i)
        links.drain(i)
    for copy in back:
        copy.wait()
    keep.wait()


def attention(member, region, gain, shards):
    dims = {"mem": lax.axis_size("mem") // 2, "lat": lax.axis_size("lat"), "lon": lax.axis_size("lon")}
    lead = (dims["mem"], 2, dims["lat"], dims["lon"])
    levels, clat, clon, width = member.shape
    bands, wins = clat // WLAT, clon // WLON
    ntok = levels * clat * clon
    gtok = ntok // bands
    slots = len(gather_keys(dims)) + len(HALO)
    anywhere = pl.BlockSpec(memory_space=pl.ANY)
    ext = (levels, clat + SH, clon + PAD, width)
    hot_ext = (clat + SH, clon + PAD, LANES)
    whole = [lead + s.shape for s in shards]
    outs = pl.pallas_call(
        functools.partial(attention_kernel, dims),
        out_shape=[
            jax.ShapeDtypeStruct(member.shape, jnp.bfloat16),
            jax.ShapeDtypeStruct((levels, clat, PAD, width), jnp.bfloat16),
            jax.ShapeDtypeStruct(whole[2], jnp.bfloat16),
            jax.ShapeDtypeStruct(whole[3], jnp.bfloat16),
        ],
        in_specs=[anywhere] + [pl.BlockSpec(memory_space=pltpu.VMEM)] * 2 + [anywhere] * 4,
        out_specs=[anywhere] * 4,
        scratch_shapes=[
            pltpu.VMEM(ext, jnp.bfloat16),
            pltpu.VMEM((4, clat, LANES), jnp.float32),
            pltpu.VMEM(ext, jnp.float32),
            pltpu.VMEM(hot_ext, jnp.float32),
            pltpu.VMEM((ntok, width), jnp.float32),
            pltpu.VMEM((ntok, LANES), jnp.float32),
            pltpu.VMEM((ntok, width), jnp.bfloat16),
            pltpu.VMEM((gtok, 3 * width), jnp.bfloat16),
            pltpu.VMEM((gtok, width), jnp.bfloat16),
            pltpu.VMEM((STAGES, gtok // wins, (LANES // HDIM) * gtok // wins), jnp.float32),
            pltpu.VMEM((STAGES, gtok // wins, (LANES // HDIM) * gtok // wins), jnp.bfloat16),
            pltpu.VMEM(whole[0], jnp.bfloat16),
            pltpu.VMEM(whole[1], jnp.bfloat16),
            pltpu.SemaphoreType.DMA((5,)),
            pltpu.SemaphoreType.DMA((slots,)),
            pltpu.SemaphoreType.DMA((slots,)),
        ],
        compiler_params=pltpu.CompilerParams(
            collective_id=0, has_side_effects=True, vmem_limit_bytes=56 * 2**20
        ),
        cost_estimate=pl.CostEstimate(
            flops=8 * ntok * width * width, bytes_accessed=4 * ntok * width, transcendentals=ntok * 4096
        ),
    )(member, region, gain, *shards)
    return outs[0], outs[1], outs[2].reshape(-1, width), outs[3].reshape(width, -1)


def mlp_kernel(resid_ref, cols_ref, gain_ref, wup_ref, wdown_ref, out_ref, acc_s):
    levels, rows, cols, width = out_ref.shape
    hidden_all = wup_ref.shape[0]
    block = resid_ref[...].astype(jnp.float32)
    came = cols_ref[...].astype(jnp.float32)
    ours = lax.broadcasted_iota(jnp.int32, came.shape, 2) >= SL
    edge = jnp.where(ours, block[:, :, :PAD], came)
    resid = jnp.concatenate([edge, block[:, :, PAD:]], axis=2).reshape(levels * rows * cols, width)
    normed = norm(resid, gain_ref[...])
    acc_s[...] = resid
    step = min(width, hidden_all)
    for at in range(0, hidden_all, step):
        pre = dot32(normed, wup_ref[pl.ds(at, step), :], NT)
        hidden = (0.5 * pre * (1.0 + lax.erf(pre * 0.5**0.5))).astype(jnp.bfloat16)
        acc_s[...] += dot32(hidden, wdown_ref[:, pl.ds(at, step)], NT)
    out_ref[...] = acc_s[...].reshape(out_ref.shape).astype(jnp.bfloat16)


def whole(shape):
    return pl.BlockSpec(shape, lambda b: (0,) * len(shape))


def body(fields, region, gain_attn, w_qkv, w_proj, gain_mlp, w_up, w_down):
    member = fields[0]
    levels, clat, clon, width = member.shape
    bands = clat // WLAT
    count = levels * clat * clon

    resid, came, wup_t, wdown_t = attention(
        member, region, gain_attn[None], [w_qkv.T, w_proj.T, w_up.T, w_down.T]
    )

    grid_block = pl.BlockSpec((levels, WLAT, clon, width), lambda b: (0, b, 0, 0))
    came_block = pl.BlockSpec((levels, WLAT, PAD, width), lambda b: (0, b, 0, 0))
    out = pl.pallas_call(
        mlp_kernel,
        grid=(bands,),
        in_specs=[grid_block, came_block, whole((1, width)), whole(wup_t.shape), whole(wdown_t.shape)],
        out_specs=grid_block,
        out_shape=jax.ShapeDtypeStruct(member.shape, jnp.bfloat16),
        scratch_shapes=[pltpu.VMEM((count // bands, width), jnp.float32)],
        compiler_params=pltpu.CompilerParams(dimension_semantics=("arbitrary",), vmem_limit_bytes=56 * 2**20),
        cost_estimate=pl.CostEstimate(
            flops=4 * count * width * wup_t.shape[0], bytes_accessed=4 * count * width, transcendentals=count * 2048
        ),
    )(resid, came, gain_mlp[None], wup_t, wdown_t)
    return out[None]


def solution(mesh):
    columns = P(None, AXES)
    in_specs = (P("mem", None, "lat", "lon", None), P("lat", "lon"), P(), columns, columns, P(), columns, columns)
    out_specs = P("mem", None, "lat", "lon", None)
    return jax.shard_map(body, mesh=mesh, in_specs=in_specs, out_specs=out_specs, check_vma=False)
```

```python
import functools

import jax
import jax.numpy as jnp
from jax import lax
from jax.experimental import pallas as pl
from jax.experimental.pallas import tpu as pltpu
from jax.sharding import PartitionSpec as P

HDIM = 32
WLAT = 6
WLON = 12
SH = 3
SL = 6
PAD = 8
LANES = 128
AXES = ("mem", "lat", "lon")
BIG = 1e9
EXP2_SCALE = 1.4426950408889634 / HDIM**0.5

eps = 1e-05

NT = (((1,), (1,)), ((), ()))
TN = (((0,), (0,)), ((), ()))
ALL = slice(None)


def dot32(a, b, dims):
    return lax.dot_general(a, b, dims, preferred_element_type=jnp.float32)


def norm(values, gain):
    average = jnp.mean(values, axis=-1, keepdims=True)
    centred = values - average
    variance = jnp.mean(centred * centred, axis=-1, keepdims=True)
    return (centred * lax.rsqrt(variance + eps) * gain).astype(jnp.bfloat16)


def window_order(bands, wins):
    rows = [(bands - 1, w) for w in range(wins - 1)]
    cols = [(b, wins - 1) for b in range(bands)]
    inner = [(b, w) for b in range(bands - 1) for w in range(wins - 1)]
    order, inner = inner[:wins], inner[wins:]
    marks = []
    for edge in (rows, cols):
        fill = -len(edge) % wins
        marks.append((len(order), len(order) + len(edge)))
        order, inner = order + edge + inner[:fill], inner[fill:]
    return order + inner, marks[0], marks[1]


def gather_plan(dims):
    last, middle = dims["lat"] - 1, dims["lat"] // 2
    ways = ("lon", "mem"), ("mem", "lon")
    fine = [(d, "all", None) for d in range(dims["lat"])]
    up = [(d,) + ways[d == middle] for d in range(dims["lat"])]
    down = [(d,) + ways[d == middle] for d in range(dims["lat"])]
    return [fine, [(None,) + ways[0]], up, down]


def spread(dims):
    return [(x, y) for x in range(dims["lon"] - 1, -1, -1) for y in range(dims["mem"] - 1, -1, -1) if x or y]


def gather_keys(dims):
    keys = []
    for i, parts in enumerate(gather_plan(dims)):
        keys += [("z", i, d) for d in range(1, dims["lat"])]
        for p, (_, a2, a3) in enumerate(parts):
            keys += [("c1", i, p)]
            if a2 == "all":
                keys += [(k, i, p, d) for d in spread(dims) for k in ("s2", "c2")]
                continue
            keys += [(k, i, p, d) for d in range(1, dims[a2]) for k in ("s2", "c2")]
            keys += [(k, i, p, d) for d in range(1, dims[a3]) for k in ("s3", "c3")]
    return keys


HALO = ("rows", "cols", "corner", "id_rows", "id_cols", "id_corner", "back_rows", "back_cols", "back_corner")
STAGES = 4


class Links:
    def __init__(self, dims, weights, send_sem, recv_sem):
        self.dims = dims
        self.plan = gather_plan(dims)
        self.weights = weights
        self.send_sem = send_sem
        self.recv_sem = recv_sem
        self.slots = {key: n for n, key in enumerate(gather_keys(dims) + list(HALO))}
        mem = lax.axis_index("mem")
        self.core = lax.rem(mem, 2)
        self.at = {"mem": lax.div(mem, 2), "lat": lax.axis_index("lat"), "lon": lax.axis_index("lon")}
        self.partner = {"mem": self.at["mem"] * 2 + 1 - self.core}

    def moved(self, axis, d):
        return lax.rem(self.at[axis] + d + self.dims[axis], self.dims[axis])

    def device(self, **offsets):
        to = {}
        for axis, d in offsets.items():
            position = self.moved(axis, d)
            to[axis] = position * 2 + self.core if axis == "mem" else position
        return to

    def copy(self, key, src, dst, to):
        slot = self.slots[key]
        return pltpu.make_async_remote_copy(
            src_ref=src,
            dst_ref=dst,
            send_sem=self.send_sem.at[slot],
            recv_sem=self.recv_sem.at[slot],
            device_id=to,
            device_id_type=pl.DeviceIdType.MESH,
        )

    def block(self, i, **where):
        index = [where.get(axis, self.at[axis]) for axis in AXES]
        return self.weights[i].at[index[0], self.core, index[1], index[2]]

    def lat_of(self, i, p):
        d = self.plan[i][p][0]
        return ALL if d is None else self.moved("lat", -d)

    def first(self, i, d):
        block = self.block(i)
        return self.copy(("z", i, d), block, block, self.device(lat=d))

    def second(self, i, p, d):
        block = self.block(i, lat=self.lat_of(i, p))
        to = dict(zip(("lon", "mem"), d)) if isinstance(d, tuple) else {self.plan[i][p][1]: d}
        return self.copy(("s2", i, p, d), block, block, self.device(**to))

    def third(self, i, p, d):
        block = self.block(i, lat=self.lat_of(i, p), **{self.plan[i][p][1]: ALL})
        return self.copy(("s3", i, p, d), block, block, self.device(**{self.plan[i][p][2]: d}))

    def cross(self, stage, i, p, d=None):
        _, a2, a3 = self.plan[i][p]
        where = {"lat": self.lat_of(i, p)}
        if stage == 2:
            for axis, far in zip(("lon", "mem"), d) if a2 == "all" else [(a2, d)]:
                where[axis] = self.moved(axis, -far)
        if stage == 3:
            where[a2] = ALL
            where[a3] = self.moved(a3, -d)
        block = self.block(i, **where)
        key = ("c1", i, p) if stage == 1 else ("c%d" % stage, i, p, d)
        return self.copy(key, block, block, self.partner)

    def peers(self, axis):
        if axis is None:
            return ()
        return spread(self.dims) if axis == "all" else range(1, self.dims[axis])

    def start_first(self, i):
        for d in self.near():
            self.first(i, d).start()

    def near(self):
        n = self.dims["lat"]
        return sorted(self.peers("lat"), key=lambda d: min(d, n - d))

    def to_second(self, i, p):
        lat, a2, _ = self.plan[i][p]
        for d in self.peers("lat"):
            if lat in (None, d):
                self.first(i, d).wait_recv()
        for d in self.peers(a2):
            self.second(i, p, d).start()
        self.cross(1, i, p).start()

    def to_third(self, i, p):
        _, a2, a3 = self.plan[i][p]
        for d in self.peers(a2):
            self.second(i, p, d).wait_recv()
        for d in self.peers(a3):
            self.third(i, p, d).start()
        for d in self.peers(a2):
            self.cross(2, i, p, d).start()

    def to_cross(self, i, p):
        for d in self.peers(self.plan[i][p][2]):
            self.third(i, p, d).wait_recv()
            self.cross(3, i, p, d).start()

    def crossings(self, i, p):
        _, a2, a3 = self.plan[i][p]
        yield self.cross(1, i, p)
        for d in self.peers(a2):
            yield self.cross(2, i, p, d)
        for d in self.peers(a3):
            yield self.cross(3, i, p, d)

    def arrive(self, i):
        for p in range(len(self.plan[i])):
            for copy in self.crossings(i, p):
                copy.wait_recv()

    def drain(self, i):
        for d in self.peers("lat"):
            self.first(i, d).wait_send()
        for p, (_, a2, a3) in enumerate(self.plan[i]):
            for d in self.peers(a2):
                self.second(i, p, d).wait_send()
            for d in self.peers(a3):
                self.third(i, p, d).wait_send()
            for copy in self.crossings(i, p):
                copy.wait_send()

    def greet(self):
        barrier = pltpu.get_barrier_semaphore()
        others = [self.partner]
        for axis in AXES:
            others += [self.device(**{axis: d}) for d in self.peers(axis)]
        others += [self.device(lon=x, mem=y) for x, y in spread(self.dims) if x and y]
        others += [self.device(lat=1, lon=1), self.device(lat=-1, lon=-1)]
        for to in others:
            pl.semaphore_signal(barrier, inc=1, device_id=to, device_id_type=pl.DeviceIdType.MESH)
        pl.semaphore_wait(barrier, len(others))


def attention_kernel(
    dims,
    x_ref,
    region_ref,
    gain_ref,
    wqkv_ref,
    wproj_ref,
    wup_ref,
    wdown_ref,
    resid_ref,
    cols_ref,
    up_ref,
    down_ref,
    ext_s,
    ids_s,
    grid_s,
    hotg_s,
    tok_s,
    hot_s,
    normed_s,
    qkv_s,
    mix_s,
    score_s,
    prob_s,
    wqkv_s,
    wproj_s,
    own_sem,
    send_sem,
    recv_sem,
):
    levels, clat, clon, width = x_ref.shape
    bands, wins = clat // WLAT, clon // WLON
    wtok = levels * WLAT * WLON
    order, (row_first, row_last), (col_first, col_last) = window_order(bands, wins)
    count = len(order)
    groups = count // wins
    gtok = wins * wtok
    chunks = dims["lat"]
    edge = list(range(row_first, row_last)) + list(range(col_first, col_last))

    links = Links(dims, [wqkv_s, wproj_s, up_ref, down_ref], send_sem, recv_sem)
    own = [
        pltpu.make_async_copy(shard, links.block(i), own_sem.at[i])
        for i, shard in enumerate([wqkv_ref, wproj_ref, wup_ref, wdown_ref])
    ]
    own.append(pltpu.make_async_copy(x_ref, ext_s.at[:, pl.ds(0, clat), pl.ds(0, clon)], own_sem.at[4]))
    for copy in own:
        copy.start()

    north = lax.broadcasted_iota(jnp.int32, (clat, clon), 0) + lax.axis_index("lat") * clat < SH
    ids_s[0] = jnp.zeros((clat, LANES), jnp.float32)
    ids_s[0, :, pl.ds(0, clon)] = (region_ref[...] + jnp.where(north, 3, 0)).astype(jnp.float32)

    top, side = pl.ds(0, SH), pl.ds(0, SL)
    body_rows, body_cols = pl.ds(0, clat), pl.ds(0, clon)
    below, beyond = pl.ds(clat, SH), pl.ds(clon, SL)
    lat_prev, lon_prev, prev = links.device(lat=-1), links.device(lon=-1), links.device(lat=-1, lon=-1)
    ids_in = [
        links.copy("id_rows", ids_s.at[0], ids_s.at[1], lat_prev),
        links.copy("id_cols", ids_s.at[0], ids_s.at[2], lon_prev),
        links.copy("id_corner", ids_s.at[0], ids_s.at[3], prev),
    ]
    rows_in = [links.copy("rows", x_ref.at[:, top], ext_s.at[:, below, body_cols], lat_prev)]
    cols_in = [
        links.copy("cols", x_ref.at[:, :, side], ext_s.at[:, body_rows, beyond], lon_prev),
        links.copy("corner", x_ref.at[:, top, side], ext_s.at[:, below, beyond], prev),
    ]

    links.greet()
    own[0].wait()
    links.start_first(0)
    links.to_second(0, 0)
    for copy in own[1:]:
        copy.wait()

    def widen(rows, cols):
        def row(r, _):
            for l in range(levels):
                grid_s[l, r, cols, :] = ext_s[l, r, cols, :].astype(jnp.float32)
            return 0

        lax.fori_loop(rows[0], rows[1], row, 0)

    def one_hot(planes, rows, cols):
        turned = planes.T
        lane = lax.broadcasted_iota(jnp.int32, (cols, LANES), 1).astype(jnp.float32)
        for r in range(rows[1] - rows[0]):
            hotg_s[rows[0] + r, pl.ds(0, cols), :] = jnp.where(turned[:cols, r : r + 1] == lane, 1.0, 0.0)

    def joined(here, there):
        lane = lax.broadcasted_iota(jnp.int32, here.shape, 1)
        return jnp.where(lane < clon, here, pltpu.roll(there, clon, 1))

    def fetch(slot):
        b, w = order[slot]
        for r in range(WLAT):
            cols = pl.ds(SL + w * WLON, WLON)
            for l in range(levels):
                to = pl.ds(slot * wtok + (l * WLAT + r) * WLON, WLON)
                tok_s[to, :] = grid_s[l, SH + b * WLAT + r, cols, :]
                hot_s[to, :] = hotg_s[SH + b * WLAT + r, cols, :]

    def norms(first, last):
        def one(s, _):
            rows = pl.ds(pl.multiple_of(s * wtok, wtok), wtok)
            normed_s[rows, :] = norm(tok_s[rows, :], gain_ref[...])
            return 0

        lax.fori_loop(first, last, one, 0)

    near = links.near()
    half = wins // 2
    widen((0, clat), pl.ds(0, clon))
    links.to_second(0, near[0])
    links.to_third(0, 0)
    links.start_first(1)
    one_hot(ids_s[0], (0, clat), clon)
    for slot in range(half):
        fetch(slot)
    for p in near[1:]:
        links.to_second(0, p)
    links.start_first(2)
    links.to_second(2, 0)
    for slot in range(half, wins):
        fetch(slot)
    for p in near:
        links.to_third(0, p)
    for copy in rows_in + ids_in:
        copy.start()
    links.start_first(3)
    links.to_second(1, 0)
    links.to_third(2, 0)
    norms(0, wins)
    for slot in range(row_last, count):
        if slot not in edge:
            fetch(slot)
    norms(row_last, col_first)
    norms(col_last, count)
    for p in [0] + near:
        links.to_cross(0, p)
    for copy in cols_in:
        copy.start()
    links.to_second(3, 0)
    links.to_second(2, near[0])
    links.arrive(0)

    def fetch_rows():
        for copy in ids_in + rows_in:
            copy.wait_recv()
        widen((clat, clat + SH), pl.ds(0, clon))
        one_hot(joined(ids_s[0], ids_s[2]), (0, clat), clon + PAD)
        one_hot(joined(ids_s[1, :PAD], ids_s[3, :PAD]), (clat, clat + SH), clon + PAD)
        for slot in range(row_first, row_last):
            fetch(slot)
        norms(row_first, row_last)

    def fetch_cols():
        for copy in cols_in:
            copy.wait_recv()
        widen((0, clat + SH), pl.ds(clon, PAD))
        for slot in range(col_first, col_last):
            fetch(slot)
        norms(col_first, col_last)

    wqkv = wqkv_s[...].reshape(3 * width, width)
    per = LANES // HDIM
    fours = width // LANES
    per_step = 4 if wins % 4 == 0 else 1
    lane_head = lax.broadcasted_iota(jnp.int32, (wtok, LANES), 1) // HDIM

    moves = {}

    def at_step(step, *move):
        moves.setdefault(step, []).append(move)

    def start_cols():
        for copy in cols_in:
            copy.start()

    at_step((0) // 2, links.to_third, 1, 0)
    for n, p in enumerate(near[1:]):
        at_step(n, links.to_second, 2, p)
    for n, p in enumerate(near):
        at_step(1 + n // 2, links.to_third, 2, p)
    for n, p in enumerate(near):
        at_step(1 + n // 2, links.to_second, 3, p)
    at_step(1, links.to_third, 3, 0)
    for n, p in enumerate(near):
        at_step(2 + n // 2, links.to_third, 3, p)
    for p in range(chunks):
        at_step(3, links.to_cross, 2, p)

    def pump(step):
        for at, todo in moves.items():

            @pl.when(step == at)
            def _():
                for move, *where in todo:
                    move(*where)

    def out_piece(slot):
        b, w = order[slot]
        for l in range(levels):
            for r in range(WLAT):
                t = pl.ds(slot * wtok + (l * WLAT + r) * WLON, WLON)
                grid_s[l, SH + b * WLAT + r, pl.ds(SL + w * WLON, WLON), :] = tok_s[t, :]

    def narrow(rows, cols):
        def row(r, _):
            for l in range(levels):
                ext_s[l, r, cols, :] = grid_s[l, r, cols, :].astype(jnp.bfloat16)
            return 0

        lax.fori_loop(rows[0], rows[1], row, 0)

    lat_next, lon_next, following = links.device(lat=1), links.device(lon=1), links.device(lat=1, lon=1)
    lower = pl.ds(SH, clat - SH)
    back = [
        links.copy("back_rows", ext_s.at[:, below, body_cols], resid_ref.at[:, top], lat_next),
        links.copy("back_cols", ext_s.at[:, lower, beyond], cols_ref.at[:, lower, pl.ds(0, SL)], lon_next),
        links.copy("back_corner", ext_s.at[:, below, beyond], cols_ref.at[:, top, pl.ds(0, SL)], following),
    ]

    def group(g, _):
        base = pl.multiple_of(g * gtok, gtok)
        mine = pl.ds(base, gtok)
        pl.when(g == row_first // wins)(fetch_rows)
        pl.when(g == col_first // wins)(fetch_cols)
        for part in range(3):
            at = pl.ds(part * width, width)
            qkv_s[:, at] = dot32(normed_s[mine, :], wqkv[part * width : (part + 1) * width], NT).astype(jnp.bfloat16)

        def windows(u, _):
            pump(g * (wins // per_step) + u)
            rows = [pl.ds(pl.multiple_of((u * per_step + j) * wtok, wtok), wtok) for j in range(per_step)]
            hots = []
            for j in range(per_step):
                at = pl.multiple_of(base + (u * per_step + j) * wtok, wtok)
                hot = hot_s[pl.ds(at, wtok), :].astype(jnp.bfloat16)
                hots.append((hot, ((hot.astype(jnp.float32) - 1.0) * BIG).astype(jnp.bfloat16)))

            def score(i):
                j, f = divmod(i, fours)
                hot, barred = hots[j]
                q = qkv_s[rows[j], pl.ds(f * LANES, LANES)]
                k = qkv_s[rows[j], pl.ds(width + f * LANES, LANES)]
                queries = [jnp.concatenate([jnp.where(lane_head == h, q, jnp.zeros_like(q)), hot], axis=1) for h in range(per)]
                score_s[i % STAGES] = dot32(jnp.concatenate([k, barred], axis=1), jnp.concatenate(queries, axis=0), NT)

            def soften(i):
                scores = score_s[i % STAGES]
                most = jnp.max(scores, axis=0, keepdims=True)
                prob_s[i % STAGES] = jnp.exp2((scores - most) * EXP2_SCALE).astype(jnp.bfloat16)

            def mix(i):
                j, f = divmod(i, fours)
                v = qkv_s[rows[j], pl.ds(2 * width + f * LANES, LANES)]
                ones = jnp.ones((wtok, HDIM // 2), jnp.bfloat16)
                mixed = dot32(jnp.concatenate([v, ones], axis=1), prob_s[i % STAGES], TN)
                heads = []
                for h in range(per):
                    at = slice(h * wtok, (h + 1) * wtok)
                    heads.append(mixed[h * HDIM : (h + 1) * HDIM, at] * (1.0 / mixed[LANES : LANES + 1, at]))
                mix_s[rows[j], pl.ds(f * LANES, LANES)] = jnp.concatenate(heads, axis=0).astype(jnp.bfloat16).T

            items = per_step * fours
            for t in range(items + 3):
                if t < items:
                    score(t)
                if 0 <= t - 2 < items:
                    soften(t - 2)
                if 0 <= t - 3 < items:
                    mix(t - 3)
            return 0

        lax.fori_loop(0, wins // per_step, windows, 0)

        @pl.when(g == 0)
        def _():
            links.to_cross(1, 0)
            links.arrive(1)

        wproj = wproj_s[...].reshape(width, width)
        attn_out = dot32(mix_s[...], wproj, NT).astype(jnp.bfloat16).astype(jnp.float32)
        tok_s[mine, :] += attn_out

        @pl.when(g == (col_last - 1) // wins)
        def _():
            for slot in edge:
                out_piece(slot)
            narrow((clat, clat + SH), pl.ds(0, clon + PAD))
            narrow((SH, clat), pl.ds(clon, PAD))
            for copy in back:
                copy.start()

        return 0

    lax.fori_loop(0, groups, group, 0)
    for slot in range(count):
        if slot not in edge:
            out_piece(slot)
    narrow((SH, clat), pl.ds(0, clon))
    keep = pltpu.make_async_copy(ext_s.at[:, lower, body_cols], resid_ref.at[:, lower], own_sem.at[0])
    keep.start()
    for p in range(chunks):
        links.to_cross(3, p)
    for copy in ids_in + rows_in + cols_in:
        copy.wait_send()
    for i in (0, 1):
        links.drain(i)
    for i in (2, 3):
        links.arrive(i)
        links.drain(i)
    for copy in back:
        copy.wait()
    keep.wait()


def attention(member, region, gain, shards):
    dims = {"mem": lax.axis_size("mem") // 2, "lat": lax.axis_size("lat"), "lon": lax.axis_size("lon")}
    lead = (dims["mem"], 2, dims["lat"], dims["lon"])
    levels, clat, clon, width = member.shape
    bands, wins = clat // WLAT, clon // WLON
    ntok = levels * clat * clon
    gtok = ntok // bands
    slots = len(gather_keys(dims)) + len(HALO)
    anywhere = pl.BlockSpec(memory_space=pl.ANY)
    ext = (levels, clat + SH, clon + PAD, width)
    hot_ext = (clat + SH, clon + PAD, LANES)
    whole = [lead + s.shape for s in shards]
    outs = pl.pallas_call(
        functools.partial(attention_kernel, dims),
        out_shape=[
            jax.ShapeDtypeStruct(member.shape, jnp.bfloat16),
            jax.ShapeDtypeStruct((levels, clat, PAD, width), jnp.bfloat16),
            jax.ShapeDtypeStruct(whole[2], jnp.bfloat16),
            jax.ShapeDtypeStruct(whole[3], jnp.bfloat16),
        ],
        in_specs=[anywhere] + [pl.BlockSpec(memory_space=pltpu.VMEM)] * 2 + [anywhere] * 4,
        out_specs=[anywhere] * 4,
        scratch_shapes=[
            pltpu.VMEM(ext, jnp.bfloat16),
            pltpu.VMEM((4, clat, LANES), jnp.float32),
            pltpu.VMEM(ext, jnp.float32),
            pltpu.VMEM(hot_ext, jnp.float32),
            pltpu.VMEM((ntok, width), jnp.float32),
            pltpu.VMEM((ntok, LANES), jnp.float32),
            pltpu.VMEM((ntok, width), jnp.bfloat16),
            pltpu.VMEM((gtok, 3 * width), jnp.bfloat16),
            pltpu.VMEM((gtok, width), jnp.bfloat16),
            pltpu.VMEM((STAGES, gtok // wins, (LANES // HDIM) * gtok // wins), jnp.float32),
            pltpu.VMEM((STAGES, gtok // wins, (LANES // HDIM) * gtok // wins), jnp.bfloat16),
            pltpu.VMEM(whole[0], jnp.bfloat16),
            pltpu.VMEM(whole[1], jnp.bfloat16),
            pltpu.SemaphoreType.DMA((5,)),
            pltpu.SemaphoreType.DMA((slots,)),
            pltpu.SemaphoreType.DMA((slots,)),
        ],
        compiler_params=pltpu.CompilerParams(
            collective_id=0, has_side_effects=True, vmem_limit_bytes=56 * 2**20
        ),
        cost_estimate=pl.CostEstimate(
            flops=8 * ntok * width * width, bytes_accessed=4 * ntok * width, transcendentals=ntok * 4096
        ),
    )(member, region, gain, *shards)
    return outs[0], outs[1], outs[2].reshape(-1, width), outs[3].reshape(width, -1)


def mlp_kernel(resid_ref, cols_ref, gain_ref, wup_ref, wdown_ref, out_ref, acc_s, normed_s, hidden_s):
    levels, rows, cols, width = out_ref.shape
    block = resid_ref[...].astype(jnp.float32)
    came = cols_ref[...].astype(jnp.float32)
    ours = lax.broadcasted_iota(jnp.int32, came.shape, 2) >= SL
    edge = jnp.where(ours, block[:, :, :PAD], came)
    resid = jnp.concatenate([edge, block[:, :, PAD:]], axis=2).reshape(levels * rows * cols, width)
    normed = norm(resid, gain_ref[...])
    acc_s[...] = resid
    tokens = levels * rows * cols
    parts = 2 if tokens % 32 == 0 else 1
    spans = [pl.ds(n * (tokens // parts), tokens // parts) for n in range(parts)]
    normed_s[...] = normed
    for span in spans:
        pre = dot32(normed_s[span, :], wup_ref[...], NT)
        hidden_s[span, :] = (0.5 * pre * (1.0 + lax.erf(pre * 0.5**0.5))).astype(jnp.bfloat16)
    for span in spans:
        acc_s[span, :] += dot32(hidden_s[span, :], wdown_ref[...], NT)
    out_ref[...] = acc_s[...].reshape(out_ref.shape).astype(jnp.bfloat16)


def whole(shape):
    return pl.BlockSpec(shape, lambda b: (0,) * len(shape))


def body(fields, region, gain_attn, w_qkv, w_proj, gain_mlp, w_up, w_down):
    member = fields[0]
    levels, clat, clon, width = member.shape
    bands = clat // WLAT
    count = levels * clat * clon

    resid, came, wup_t, wdown_t = attention(
        member, region, gain_attn[None], [w_qkv.T, w_proj.T, w_up.T, w_down.T]
    )

    grid_block = pl.BlockSpec((levels, WLAT, clon, width), lambda b: (0, b, 0, 0))
    came_block = pl.BlockSpec((levels, WLAT, PAD, width), lambda b: (0, b, 0, 0))
    out = pl.pallas_call(
        mlp_kernel,
        grid=(bands,),
        in_specs=[grid_block, came_block, whole((1, width)), whole(wup_t.shape), whole(wdown_t.shape)],
        out_specs=grid_block,
        out_shape=jax.ShapeDtypeStruct(member.shape, jnp.bfloat16),
        scratch_shapes=[
            pltpu.VMEM((count // bands, width), jnp.float32),
            pltpu.VMEM((count // bands, width), jnp.bfloat16),
            pltpu.VMEM((count // bands, wup_t.shape[0]), jnp.bfloat16),
        ],
        compiler_params=pltpu.CompilerParams(dimension_semantics=("arbitrary",), vmem_limit_bytes=56 * 2**20),
        cost_estimate=pl.CostEstimate(
            flops=4 * count * width * wup_t.shape[0], bytes_accessed=4 * count * width, transcendentals=count * 2048
        ),
    )(resid, came, gain_mlp[None], wup_t, wdown_t)
    return out[None]


def solution(mesh):
    columns = P(None, AXES)
    in_specs = (P("mem", None, "lat", "lon", None), P("lat", "lon"), P(), columns, columns, P(), columns, columns)
    out_specs = P("mem", None, "lat", "lon", None)
    return jax.shard_map(body, mesh=mesh, in_specs=in_specs, out_specs=out_specs, check_vma=False)
```

```python
import functools

import jax
import jax.numpy as jnp
from jax import lax
from jax.experimental import pallas as pl
from jax.experimental.pallas import tpu as pltpu
from jax.sharding import PartitionSpec as P

HDIM = 32
WLAT = 6
WLON = 12
SH = 3
SL = 6
PAD = 8
LANES = 128
AXES = ("mem", "lat", "lon")
BIG = 1e9
EXP2_SCALE = 1.4426950408889634 / HDIM**0.5

eps = 1e-05

NT = (((1,), (1,)), ((), ()))
TN = (((0,), (0,)), ((), ()))
ALL = slice(None)


def dot32(a, b, dims):
    return lax.dot_general(a, b, dims, preferred_element_type=jnp.float32)


def norm(values, gain):
    average = jnp.mean(values, axis=-1, keepdims=True)
    centred = values - average
    variance = jnp.mean(centred * centred, axis=-1, keepdims=True)
    return (centred * lax.rsqrt(variance + eps) * gain).astype(jnp.bfloat16)


def window_order(bands, wins):
    rows = [(bands - 1, w) for w in range(wins - 1)]
    cols = [(b, wins - 1) for b in range(bands)]
    inner = [(b, w) for b in range(bands - 1) for w in range(wins - 1)]
    order, inner = inner[:wins], inner[wins:]
    marks = []
    for edge in (rows, cols):
        fill = -len(edge) % wins
        marks.append((len(order), len(order) + len(edge)))
        order, inner = order + edge + inner[:fill], inner[fill:]
    return order + inner, marks[0], marks[1]


def gather_plan(dims):
    last, middle = dims["lat"] - 1, dims["lat"] // 2
    ways = ("lon", "mem"), ("mem", "lon")
    fine = [(d, "all", None) for d in range(dims["lat"])]
    up = [(d,) + ways[d == middle] for d in range(dims["lat"])]
    down = [(d,) + ways[d == middle] for d in range(dims["lat"])]
    return [fine, [(None,) + ways[0]], up, down]


def spread(dims):
    return [(x, y) for x in range(dims["lon"] - 1, -1, -1) for y in range(dims["mem"] - 1, -1, -1) if x or y]


def gather_keys(dims):
    keys = []
    for i, parts in enumerate(gather_plan(dims)):
        keys += [("z", i, d) for d in range(1, dims["lat"])]
        for p, (_, a2, a3) in enumerate(parts):
            keys += [("c1", i, p)]
            if a2 == "all":
                keys += [(k, i, p, d) for d in spread(dims) for k in ("s2", "c2")]
                continue
            keys += [(k, i, p, d) for d in range(1, dims[a2]) for k in ("s2", "c2")]
            keys += [(k, i, p, d) for d in range(1, dims[a3]) for k in ("s3", "c3")]
    return keys


HALO = ("rows", "cols", "corner", "id_rows", "id_cols", "id_corner", "back_rows", "back_cols", "back_corner")
STAGES = 4


class Links:
    def __init__(self, dims, weights, send_sem, recv_sem):
        self.dims = dims
        self.plan = gather_plan(dims)
        self.weights = weights
        self.send_sem = send_sem
        self.recv_sem = recv_sem
        self.slots = {key: n for n, key in enumerate(gather_keys(dims) + list(HALO))}
        mem = lax.axis_index("mem")
        self.core = lax.rem(mem, 2)
        self.at = {"mem": lax.div(mem, 2), "lat": lax.axis_index("lat"), "lon": lax.axis_index("lon")}
        self.partner = {"mem": self.at["mem"] * 2 + 1 - self.core}

    def moved(self, axis, d):
        return lax.rem(self.at[axis] + d + self.dims[axis], self.dims[axis])

    def device(self, **offsets):
        to = {}
        for axis, d in offsets.items():
            position = self.moved(axis, d)
            to[axis] = position * 2 + self.core if axis == "mem" else position
        return to

    def copy(self, key, src, dst, to):
        slot = self.slots[key]
        return pltpu.make_async_remote_copy(
            src_ref=src,
            dst_ref=dst,
            send_sem=self.send_sem.at[slot],
            recv_sem=self.recv_sem.at[slot],
            device_id=to,
            device_id_type=pl.DeviceIdType.MESH,
        )

    def block(self, i, **where):
        index = [where.get(axis, self.at[axis]) for axis in AXES]
        return self.weights[i].at[index[0], self.core, index[1], index[2]]

    def lat_of(self, i, p):
        d = self.plan[i][p][0]
        return ALL if d is None else self.moved("lat", -d)

    def first(self, i, d):
        block = self.block(i)
        return self.copy(("z", i, d), block, block, self.device(lat=d))

    def second(self, i, p, d):
        block = self.block(i, lat=self.lat_of(i, p))
        to = dict(zip(("lon", "mem"), d)) if isinstance(d, tuple) else {self.plan[i][p][1]: d}
        return self.copy(("s2", i, p, d), block, block, self.device(**to))

    def third(self, i, p, d):
        block = self.block(i, lat=self.lat_of(i, p), **{self.plan[i][p][1]: ALL})
        return self.copy(("s3", i, p, d), block, block, self.device(**{self.plan[i][p][2]: d}))

    def cross(self, stage, i, p, d=None):
        _, a2, a3 = self.plan[i][p]
        where = {"lat": self.lat_of(i, p)}
        if stage == 2:
            for axis, far in zip(("lon", "mem"), d) if a2 == "all" else [(a2, d)]:
                where[axis] = self.moved(axis, -far)
        if stage == 3:
            where[a2] = ALL
            where[a3] = self.moved(a3, -d)
        block = self.block(i, **where)
        key = ("c1", i, p) if stage == 1 else ("c%d" % stage, i, p, d)
        return self.copy(key, block, block, self.partner)

    def peers(self, axis):
        if axis is None:
            return ()
        return spread(self.dims) if axis == "all" else range(1, self.dims[axis])

    def start_first(self, i):
        for d in self.near():
            self.first(i, d).start()

    def near(self):
        n = self.dims["lat"]
        return sorted(self.peers("lat"), key=lambda d: min(d, n - d))

    def to_second(self, i, p):
        lat, a2, _ = self.plan[i][p]
        for d in self.peers("lat"):
            if lat in (None, d):
                self.first(i, d).wait_recv()
        for d in self.peers(a2):
            self.second(i, p, d).start()
        self.cross(1, i, p).start()

    def to_third(self, i, p):
        _, a2, a3 = self.plan[i][p]
        for d in self.peers(a2):
            self.second(i, p, d).wait_recv()
        for d in self.peers(a3):
            self.third(i, p, d).start()
        for d in self.peers(a2):
            self.cross(2, i, p, d).start()

    def to_cross(self, i, p):
        for d in self.peers(self.plan[i][p][2]):
            self.third(i, p, d).wait_recv()
            self.cross(3, i, p, d).start()

    def crossings(self, i, p):
        _, a2, a3 = self.plan[i][p]
        yield self.cross(1, i, p)
        for d in self.peers(a2):
            yield self.cross(2, i, p, d)
        for d in self.peers(a3):
            yield self.cross(3, i, p, d)

    def arrive(self, i):
        for p in range(len(self.plan[i])):
            for copy in self.crossings(i, p):
                copy.wait_recv()

    def drain(self, i):
        for d in self.peers("lat"):
            self.first(i, d).wait_send()
        for p, (_, a2, a3) in enumerate(self.plan[i]):
            for d in self.peers(a2):
                self.second(i, p, d).wait_send()
            for d in self.peers(a3):
                self.third(i, p, d).wait_send()
            for copy in self.crossings(i, p):
                copy.wait_send()

    def greet(self):
        barrier = pltpu.get_barrier_semaphore()
        others = [self.partner]
        for axis in AXES:
            others += [self.device(**{axis: d}) for d in self.peers(axis)]
        others += [self.device(lon=x, mem=y) for x, y in spread(self.dims) if x and y]
        others += [self.device(lat=1, lon=1), self.device(lat=-1, lon=-1)]
        for to in others:
            pl.semaphore_signal(barrier, inc=1, device_id=to, device_id_type=pl.DeviceIdType.MESH)
        pl.semaphore_wait(barrier, len(others))


def attention_kernel(
    dims,
    x_ref,
    region_ref,
    gain_ref,
    wqkv_ref,
    wproj_ref,
    wup_ref,
    wdown_ref,
    resid_ref,
    cols_ref,
    up_ref,
    down_ref,
    ext_s,
    ids_s,
    grid_s,
    hotg_s,
    tok_s,
    hot_s,
    normed_s,
    qkv_s,
    mix_s,
    score_s,
    prob_s,
    wqkv_s,
    wproj_s,
    own_sem,
    send_sem,
    recv_sem,
):
    levels, clat, clon, width = x_ref.shape
    bands, wins = clat // WLAT, clon // WLON
    wtok = levels * WLAT * WLON
    order, (row_first, row_last), (col_first, col_last) = window_order(bands, wins)
    count = len(order)
    groups = count // wins
    gtok = wins * wtok
    chunks = dims["lat"]
    edge = list(range(row_first, row_last)) + list(range(col_first, col_last))

    links = Links(dims, [wqkv_s, wproj_s, up_ref, down_ref], send_sem, recv_sem)
    own = [
        pltpu.make_async_copy(shard, links.block(i), own_sem.at[i])
        for i, shard in enumerate([wqkv_ref, wproj_ref, wup_ref, wdown_ref])
    ]
    own.append(pltpu.make_async_copy(x_ref, ext_s.at[:, pl.ds(0, clat), pl.ds(0, clon)], own_sem.at[4]))
    for copy in own:
        copy.start()

    north = lax.broadcasted_iota(jnp.int32, (clat, clon), 0) + lax.axis_index("lat") * clat < SH
    ids_s[0] = jnp.zeros((clat, LANES), jnp.float32)
    ids_s[0, :, pl.ds(0, clon)] = (region_ref[...] + jnp.where(north, 3, 0)).astype(jnp.float32)

    top, side = pl.ds(0, SH), pl.ds(0, SL)
    body_rows, body_cols = pl.ds(0, clat), pl.ds(0, clon)
    below, beyond = pl.ds(clat, SH), pl.ds(clon, SL)
    lat_prev, lon_prev, prev = links.device(lat=-1), links.device(lon=-1), links.device(lat=-1, lon=-1)
    ids_in = [
        links.copy("id_rows", ids_s.at[0], ids_s.at[1], lat_prev),
        links.copy("id_cols", ids_s.at[0], ids_s.at[2], lon_prev),
        links.copy("id_corner", ids_s.at[0], ids_s.at[3], prev),
    ]
    rows_in = [links.copy("rows", x_ref.at[:, top], ext_s.at[:, below, body_cols], lat_prev)]
    cols_in = [
        links.copy("cols", x_ref.at[:, :, side], ext_s.at[:, body_rows, beyond], lon_prev),
        links.copy("corner", x_ref.at[:, top, side], ext_s.at[:, below, beyond], prev),
    ]

    links.greet()
    own[0].wait()
    links.start_first(0)
    links.to_second(0, 0)
    for copy in own[1:]:
        copy.wait()

    def widen(rows, cols):
        def row(r, _):
            for l in range(levels):
                grid_s[l, r, cols, :] = ext_s[l, r, cols, :].astype(jnp.float32)
            return 0

        lax.fori_loop(rows[0], rows[1], row, 0)

    def one_hot(planes, rows, cols):
        turned = planes.T
        lane = lax.broadcasted_iota(jnp.int32, (cols, LANES), 1).astype(jnp.float32)
        for r in range(rows[1] - rows[0]):
            hotg_s[rows[0] + r, pl.ds(0, cols), :] = jnp.where(turned[:cols, r : r + 1] == lane, 1.0, 0.0)

    def joined(here, there):
        lane = lax.broadcasted_iota(jnp.int32, here.shape, 1)
        return jnp.where(lane < clon, here, pltpu.roll(there, clon, 1))

    def fetch(slot):
        b, w = order[slot]
        for r in range(WLAT):
            cols = pl.ds(SL + w * WLON, WLON)
            for l in range(levels):
                to = pl.ds(slot * wtok + (l * WLAT + r) * WLON, WLON)
                tok_s[to, :] = grid_s[l, SH + b * WLAT + r, cols, :]
                hot_s[to, :] = hotg_s[SH + b * WLAT + r, cols, :]

    def norms(first, last):
        def one(s, _):
            rows = pl.ds(pl.multiple_of(s * wtok, wtok), wtok)
            normed_s[rows, :] = norm(tok_s[rows, :], gain_ref[...])
            return 0

        lax.fori_loop(first, last, one, 0)

    near = links.near()
    half = wins // 2
    widen((0, clat), pl.ds(0, clon))
    links.to_second(0, near[0])
    links.to_third(0, 0)
    links.start_first(1)
    one_hot(ids_s[0], (0, clat), clon)
    for slot in range(half):
        fetch(slot)
    for p in near[1:]:
        links.to_second(0, p)
    links.start_first(2)
    links.to_second(2, 0)
    for slot in range(half, wins):
        fetch(slot)
    for p in near:
        links.to_third(0, p)
    for copy in rows_in + ids_in:
        copy.start()
    links.start_first(3)
    links.to_second(1, 0)
    links.to_third(2, 0)
    norms(0, wins)
    for slot in range(row_last, count):
        if slot not in edge:
            fetch(slot)
    norms(row_last, col_first)
    norms(col_last, count)
    for p in [0] + near:
        links.to_cross(0, p)
    for copy in cols_in:
        copy.start()
    links.to_second(3, 0)
    links.to_second(2, near[0])
    links.arrive(0)

    def fetch_rows():
        for copy in ids_in + rows_in:
            copy.wait_recv()
        widen((clat, clat + SH), pl.ds(0, clon))
        one_hot(joined(ids_s[0], ids_s[2]), (0, clat), clon + PAD)
        one_hot(joined(ids_s[1, :PAD], ids_s[3, :PAD]), (clat, clat + SH), clon + PAD)
        for slot in range(row_first, row_last):
            fetch(slot)
        norms(row_first, row_last)

    def fetch_cols():
        for copy in cols_in:
            copy.wait_recv()
        widen((0, clat + SH), pl.ds(clon, PAD))
        for slot in range(col_first, col_last):
            fetch(slot)
        norms(col_first, col_last)

    wqkv = wqkv_s[...].reshape(3 * width, width)
    per = LANES // HDIM
    fours = width // LANES
    per_step = 4 if wins % 4 == 0 else 1
    lane_head = lax.broadcasted_iota(jnp.int32, (wtok, LANES), 1) // HDIM

    moves = {}

    def at_step(step, *move):
        moves.setdefault(step, []).append(move)

    def start_cols():
        for copy in cols_in:
            copy.start()

    at_step((0) // 2, links.to_third, 1, 0)
    for n, p in enumerate(near[1:]):
        at_step(n, links.to_second, 2, p)
    for n, p in enumerate(near):
        at_step(1 + n // 2, links.to_third, 2, p)
    for n, p in enumerate(near):
        at_step(1 + n // 2, links.to_second, 3, p)
    at_step(1, links.to_third, 3, 0)
    for n, p in enumerate(near):
        at_step(2 + (n > 0), links.to_third, 3, p)

    def pump(step):
        for at, todo in moves.items():

            @pl.when(step == at)
            def _():
                for move, *where in todo:
                    move(*where)

    def out_piece(slot):
        b, w = order[slot]
        for l in range(levels):
            for r in range(WLAT):
                t = pl.ds(slot * wtok + (l * WLAT + r) * WLON, WLON)
                grid_s[l, SH + b * WLAT + r, pl.ds(SL + w * WLON, WLON), :] = tok_s[t, :]

    inner = [slot for slot in range(count) if slot not in edge]
    ready = [slot for slot in inner if slot < col_first]

    def out_ready():
        for slot in ready:
            out_piece(slot)

    moves.setdefault(col_first // wins * (wins // per_step), []).insert(0, (out_ready,))

    def narrow(rows, cols):
        def row(r, _):
            for l in range(levels):
                ext_s[l, r, cols, :] = grid_s[l, r, cols, :].astype(jnp.bfloat16)
            return 0

        lax.fori_loop(rows[0], rows[1], row, 0)

    lat_next, lon_next, following = links.device(lat=1), links.device(lon=1), links.device(lat=1, lon=1)
    lower = pl.ds(SH, clat - SH)
    back = [
        links.copy("back_rows", ext_s.at[:, below, body_cols], resid_ref.at[:, top], lat_next),
        links.copy("back_cols", ext_s.at[:, lower, beyond], cols_ref.at[:, lower, pl.ds(0, SL)], lon_next),
        links.copy("back_corner", ext_s.at[:, below, beyond], cols_ref.at[:, top, pl.ds(0, SL)], following),
    ]

    def group(g, _):
        base = pl.multiple_of(g * gtok, gtok)
        mine = pl.ds(base, gtok)
        pl.when(g == row_first // wins)(fetch_rows)
        pl.when(g == col_first // wins)(fetch_cols)
        for part in range(3):
            at = pl.ds(part * width, width)
            qkv_s[:, at] = dot32(normed_s[mine, :], wqkv[part * width : (part + 1) * width], NT).astype(jnp.bfloat16)

        def windows(u, _):
            pump(g * (wins // per_step) + u)
            rows = [pl.ds(pl.multiple_of((u * per_step + j) * wtok, wtok), wtok) for j in range(per_step)]
            hots = []
            for j in range(per_step):
                at = pl.multiple_of(base + (u * per_step + j) * wtok, wtok)
                hot = hot_s[pl.ds(at, wtok), :].astype(jnp.bfloat16)
                hots.append((hot, ((hot.astype(jnp.float32) - 1.0) * BIG).astype(jnp.bfloat16)))

            def score(i):
                j, f = divmod(i, fours)
                hot, barred = hots[j]
                q = qkv_s[rows[j], pl.ds(f * LANES, LANES)]
                k = qkv_s[rows[j], pl.ds(width + f * LANES, LANES)]
                queries = [jnp.concatenate([jnp.where(lane_head == h, q, jnp.zeros_like(q)), hot], axis=1) for h in range(per)]
                score_s[i % STAGES] = dot32(jnp.concatenate([k, barred], axis=1), jnp.concatenate(queries, axis=0), NT)

            def soften(i):
                scores = score_s[i % STAGES]
                most = jnp.max(scores, axis=0, keepdims=True)
                prob_s[i % STAGES] = jnp.exp2((scores - most) * EXP2_SCALE).astype(jnp.bfloat16)

            def mix(i):
                j, f = divmod(i, fours)
                v = qkv_s[rows[j], pl.ds(2 * width + f * LANES, LANES)]
                ones = jnp.ones((wtok, HDIM // 2), jnp.bfloat16)
                mixed = dot32(jnp.concatenate([v, ones], axis=1), prob_s[i % STAGES], TN)
                heads = []
                for h in range(per):
                    at = slice(h * wtok, (h + 1) * wtok)
                    heads.append(mixed[h * HDIM : (h + 1) * HDIM, at] * (1.0 / mixed[LANES : LANES + 1, at]))
                mix_s[rows[j], pl.ds(f * LANES, LANES)] = jnp.concatenate(heads, axis=0).astype(jnp.bfloat16).T

            items = per_step * fours
            for t in range(items + 3):
                if t < items:
                    score(t)
                if 0 <= t - 2 < items:
                    soften(t - 2)
                if 0 <= t - 3 < items:
                    mix(t - 3)
            return 0

        lax.fori_loop(0, wins // per_step, windows, 0)

        @pl.when(g == 0)
        def _():
            links.to_cross(1, 0)
            links.arrive(1)

        wproj = wproj_s[...].reshape(width, width)
        attn_out = dot32(mix_s[...], wproj, NT).astype(jnp.bfloat16).astype(jnp.float32)
        tok_s[mine, :] += attn_out

        @pl.when(g == (col_last - 1) // wins)
        def _():
            for slot in edge:
                out_piece(slot)
            narrow((clat, clat + SH), pl.ds(0, clon + PAD))
            narrow((SH, clat), pl.ds(clon, PAD))
            for copy in back:
                copy.start()

        return 0

    lax.fori_loop(0, groups, group, 0)
    for slot in inner:
        if slot not in ready:
            out_piece(slot)
    narrow((SH, clat), pl.ds(0, clon))
    keep = pltpu.make_async_copy(ext_s.at[:, lower, body_cols], resid_ref.at[:, lower], own_sem.at[0])
    keep.start()
    for p in range(chunks):
        links.to_cross(2, p)
    for p in range(chunks):
        links.to_cross(3, p)
    for copy in ids_in + rows_in + cols_in:
        copy.wait_send()
    for i in (0, 1):
        links.drain(i)
    for i in (2, 3):
        links.arrive(i)
        links.drain(i)
    for copy in back:
        copy.wait()
    keep.wait()


def attention(member, region, gain, shards):
    dims = {"mem": lax.axis_size("mem") // 2, "lat": lax.axis_size("lat"), "lon": lax.axis_size("lon")}
    lead = (dims["mem"], 2, dims["lat"], dims["lon"])
    levels, clat, clon, width = member.shape
    bands, wins = clat // WLAT, clon // WLON
    ntok = levels * clat * clon
    gtok = ntok // bands
    slots = len(gather_keys(dims)) + len(HALO)
    anywhere = pl.BlockSpec(memory_space=pl.ANY)
    ext = (levels, clat + SH, clon + PAD, width)
    hot_ext = (clat + SH, clon + PAD, LANES)
    whole = [lead + s.shape for s in shards]
    outs = pl.pallas_call(
        functools.partial(attention_kernel, dims),
        out_shape=[
            jax.ShapeDtypeStruct(member.shape, jnp.bfloat16),
            jax.ShapeDtypeStruct((levels, clat, PAD, width), jnp.bfloat16),
            jax.ShapeDtypeStruct(whole[2], jnp.bfloat16),
            jax.ShapeDtypeStruct(whole[3], jnp.bfloat16),
        ],
        in_specs=[anywhere] + [pl.BlockSpec(memory_space=pltpu.VMEM)] * 2 + [anywhere] * 4,
        out_specs=[anywhere] * 4,
        scratch_shapes=[
            pltpu.VMEM(ext, jnp.bfloat16),
            pltpu.VMEM((4, clat, LANES), jnp.float32),
            pltpu.VMEM(ext, jnp.float32),
            pltpu.VMEM(hot_ext, jnp.float32),
            pltpu.VMEM((ntok, width), jnp.float32),
            pltpu.VMEM((ntok, LANES), jnp.float32),
            pltpu.VMEM((ntok, width), jnp.bfloat16),
            pltpu.VMEM((gtok, 3 * width), jnp.bfloat16),
            pltpu.VMEM((gtok, width), jnp.bfloat16),
            pltpu.VMEM((STAGES, gtok // wins, (LANES // HDIM) * gtok // wins), jnp.float32),
            pltpu.VMEM((STAGES, gtok // wins, (LANES // HDIM) * gtok // wins), jnp.bfloat16),
            pltpu.VMEM(whole[0], jnp.bfloat16),
            pltpu.VMEM(whole[1], jnp.bfloat16),
            pltpu.SemaphoreType.DMA((5,)),
            pltpu.SemaphoreType.DMA((slots,)),
            pltpu.SemaphoreType.DMA((slots,)),
        ],
        compiler_params=pltpu.CompilerParams(
            collective_id=0, has_side_effects=True, vmem_limit_bytes=56 * 2**20
        ),
        cost_estimate=pl.CostEstimate(
            flops=8 * ntok * width * width, bytes_accessed=4 * ntok * width, transcendentals=ntok * 4096
        ),
    )(member, region, gain, *shards)
    return outs[0], outs[1], outs[2].reshape(-1, width), outs[3].reshape(width, -1)


def mlp_kernel(resid_ref, cols_ref, gain_ref, wup_ref, wdown_ref, out_ref, acc_s, normed_s, hidden_s):
    levels, rows, cols, width = out_ref.shape
    block = resid_ref[...].astype(jnp.float32)
    came = cols_ref[...].astype(jnp.float32)
    ours = lax.broadcasted_iota(jnp.int32, came.shape, 2) >= SL
    edge = jnp.where(ours, block[:, :, :PAD], came)
    resid = jnp.concatenate([edge, block[:, :, PAD:]], axis=2).reshape(levels * rows * cols, width)
    normed = norm(resid, gain_ref[...])
    acc_s[...] = resid
    tokens = levels * rows * cols
    parts = 2 if tokens % 32 == 0 else 1
    spans = [pl.ds(n * (tokens // parts), tokens // parts) for n in range(parts)]
    normed_s[...] = normed
    for span in spans:
        pre = dot32(normed_s[span, :], wup_ref[...], NT)
        hidden_s[span, :] = (0.5 * pre * (1.0 + lax.erf(pre * 0.5**0.5))).astype(jnp.bfloat16)
    for span in spans:
        acc_s[span, :] += dot32(hidden_s[span, :], wdown_ref[...], NT)
    out_ref[...] = acc_s[...].reshape(out_ref.shape).astype(jnp.bfloat16)


def whole(shape):
    return pl.BlockSpec(shape, lambda b: (0,) * len(shape))


def body(fields, region, gain_attn, w_qkv, w_proj, gain_mlp, w_up, w_down):
    member = fields[0]
    levels, clat, clon, width = member.shape
    bands = clat // WLAT
    count = levels * clat * clon

    resid, came, wup_t, wdown_t = attention(
        member, region, gain_attn[None], [w_qkv.T, w_proj.T, w_up.T, w_down.T]
    )

    grid_block = pl.BlockSpec((levels, WLAT, clon, width), lambda b: (0, b, 0, 0))
    came_block = pl.BlockSpec((levels, WLAT, PAD, width), lambda b: (0, b, 0, 0))
    out = pl.pallas_call(
        mlp_kernel,
        grid=(bands,),
        in_specs=[grid_block, came_block, whole((1, width)), whole(wup_t.shape), whole(wdown_t.shape)],
        out_specs=grid_block,
        out_shape=jax.ShapeDtypeStruct(member.shape, jnp.bfloat16),
        scratch_shapes=[
            pltpu.VMEM((count // bands, width), jnp.float32),
            pltpu.VMEM((count // bands, width), jnp.bfloat16),
            pltpu.VMEM((count // bands, wup_t.shape[0]), jnp.bfloat16),
        ],
        compiler_params=pltpu.CompilerParams(dimension_semantics=("arbitrary",), vmem_limit_bytes=56 * 2**20),
        cost_estimate=pl.CostEstimate(
            flops=4 * count * width * wup_t.shape[0], bytes_accessed=4 * count * width, transcendentals=count * 2048
        ),
    )(resid, came, gain_mlp[None], wup_t, wdown_t)
    return out[None]


def solution(mesh):
    columns = P(None, AXES)
    in_specs = (P("mem", None, "lat", "lon", None), P("lat", "lon"), P(), columns, columns, P(), columns, columns)
    out_specs = P("mem", None, "lat", "lon", None)
    return jax.shard_map(body, mesh=mesh, in_specs=in_specs, out_specs=out_specs, check_vma=False)
```
